8 devices in a mesh: tp: 4 (over z, y, x), cp: 2 (over core).
Axes of the slice: x: 2, y: 2, z: 1, core: 2. Of those that a mesh axis runs over, the one named last changes fastest.
Arguments:
- hidden: bfloat16 [12, 1024, 2560], P(None, 'cp')
- grad_out: bfloat16 [12, 1024, 2560], P(None, 'cp')
- w_dq: bfloat16 [2560, 768], replicated
- g_q: bfloat16 [768], replicated
- w_dkv: bfloat16 [2560, 288], replicated
- g_kv: bfloat16 [256], replicated
- w_uq: bfloat16 [768, 40, 96], P(None, 'tp')
- w_uk: bfloat16 [256, 40, 64], P(None, 'tp')
- w_uv: bfloat16 [256, 40, 64], P(None, 'tp')
- w_o: bfloat16 [40, 64, 2560], P('tp')
Outputs:
- output 1: bfloat16 [12, 1024, 2560], P(None, 'cp')
- output 2: bfloat16 [12, 1024, 2560], P(None, 'cp')
- output 3: float32 [2560, 768], replicated
- output 4: float32 [768], replicated
- output 5: float32 [2560, 288], replicated
- output 6: float32 [256], replicated
- output 7: float32 [768, 40, 96], P(None, 'tp')
- output 8: float32 [256, 40, 64], P(None, 'tp')
- output 9: float32 [256, 40, 64], P(None, 'tp')
- output 10: float32 [40, 64, 2560], P('tp')
All inputs are finite; a program needn't handle non-finite values.
Results may differ from the reference program's by a relative error of at most 0.0156823.
Values are sent between devices in bfloat16 or wider.
A program may use at most 1 GiB of HBM per device.

```python
import jax
import jax.numpy as jnp
from jax import lax

D = 2560
HEADS = 40
Q_LORA = 768
KV_LORA = 256
NOPE = 64
ROPE = 32
VHEAD = 64
BATCH = 12
SEQ_DEV = 512
CP = 2
QBLK = 64
THETA = 10000

SEQ = CP * SEQ_DEV
HALF_LEN = SEQ_DEV // 2
QK_DIM = NOPE + ROPE
EPS = 1e-6
NEG_BIG = -1e30


def token_positions():
    token_idx = jnp.arange(SEQ, dtype=jnp.int32)
    cp_rank = token_idx // SEQ_DEV
    local_idx = token_idx % SEQ_DEV
    block_id = jnp.where(local_idx < HALF_LEN, cp_rank, 2 * CP - 1 - cp_rank)
    return block_id * HALF_LEN + local_idx % HALF_LEN


def rope_tables(positions):
    inv_freq = 1.0 / (THETA ** (jnp.arange(ROPE // 2, dtype=jnp.float32) * 2.0 / ROPE))
    angles = positions.astype(jnp.float32)[:, None] * inv_freq[None, :]
    return jnp.cos(angles), jnp.sin(angles)


def apply_rope(values, cos_tab, sin_tab):
    half_dim = values.shape[-1] // 2
    lead_half = values[..., :half_dim]
    tail_half = values[..., half_dim:]
    return jnp.concatenate([lead_half * cos_tab - tail_half * sin_tab, tail_half * cos_tab + lead_half * sin_tab], axis=-1)


def rms_norm(raw_vals, gain_vec):
    raw_f32 = raw_vals.astype(jnp.float32)
    inv_rms = lax.rsqrt(jnp.mean(raw_f32 * raw_f32, axis=-1, keepdims=True) + EPS)
    return (raw_f32 * inv_rms * gain_vec).astype(jnp.bfloat16)


def attention(q_nope, q_pe, k_nope, k_pe, v_heads, positions):
    kn_f32 = k_nope.astype(jnp.float32)
    kp_f32 = k_pe.astype(jnp.float32)
    v_f32 = v_heads.astype(jnp.float32)
    n_blocks = SEQ // QBLK
    qn_blocks = jnp.moveaxis(q_nope.reshape(BATCH, n_blocks, QBLK, HEADS, NOPE), 1, 0)
    qp_blocks = jnp.moveaxis(q_pe.reshape(BATCH, n_blocks, QBLK, HEADS, ROPE), 1, 0)
    pos_blocks = positions.reshape(n_blocks, QBLK)

    def one_block(block_args):
        qn_blk, qp_blk, q_pos = block_args
        scores = jnp.einsum('bqhn,bkhn->bhqk', qn_blk.astype(jnp.float32), kn_f32) + jnp.einsum('bqhr,bkr->bhqk', qp_blk.astype(jnp.float32), kp_f32)
        scores = jnp.where(positions[None, :] <= q_pos[:, None], scores * QK_DIM ** -0.5, NEG_BIG)
        weights = jax.nn.softmax(scores, axis=-1)
        return jnp.einsum('bhqk,bkhv->bqhv', weights, v_f32).astype(jnp.bfloat16)

    out_blocks = lax.map(jax.checkpoint(one_block), (qn_blocks, qp_blocks, pos_blocks))
    return jnp.moveaxis(out_blocks, 0, 1).reshape(BATCH, SEQ, HEADS, VHEAD)


def forward(hidden, w_dq, g_q, w_dkv, g_kv, w_uq, w_uk, w_uv, w_o):
    positions = token_positions()
    cos_tab, sin_tab = rope_tables(positions)
    hidden_f32 = hidden.astype(jnp.float32)
    cq_raw = jnp.einsum('btd,dq->btq', hidden_f32, w_dq).astype(jnp.bfloat16)
    kv_raw = jnp.einsum('btd,dc->btc', hidden_f32, w_dkv).astype(jnp.bfloat16)
    c_q = rms_norm(cq_raw, g_q)
    c_kv = rms_norm(kv_raw[..., :KV_LORA], g_kv)
    k_pe = apply_rope(kv_raw[..., KV_LORA:].astype(jnp.float32), cos_tab, sin_tab).astype(jnp.bfloat16)
    q_all = jnp.einsum('btq,qhe->bthe', c_q.astype(jnp.float32), w_uq).astype(jnp.bfloat16)
    q_nope = q_all[..., :NOPE]
    q_pe = apply_rope(q_all[..., NOPE:].astype(jnp.float32), cos_tab[:, None, :], sin_tab[:, None, :]).astype(jnp.bfloat16)
    k_nope = jnp.einsum('btc,chn->bthn', c_kv.astype(jnp.float32), w_uk).astype(jnp.bfloat16)
    v_heads = jnp.einsum('btc,chv->bthv', c_kv.astype(jnp.float32), w_uv).astype(jnp.bfloat16)
    o_heads = attention(q_nope, q_pe, k_nope, k_pe, v_heads, positions)
    return jnp.einsum('bthv,hvd->btd', o_heads.astype(jnp.float32), w_o).astype(jnp.bfloat16)


def setup_inputs(seed: int = 0) -> dict:
    rng_keys = jax.random.split(jax.random.key(seed), 10)

    def normal_weight(rng_key, arr_shape, fan_in):
        return (jax.random.normal(rng_key, arr_shape, jnp.float32) * fan_in ** -0.5).astype(jnp.bfloat16)

    return {
        'hidden': jax.random.normal(rng_keys[0], (BATCH, SEQ, D), jnp.float32).astype(jnp.bfloat16),
        'grad_out': jax.random.normal(rng_keys[1], (BATCH, SEQ, D), jnp.float32).astype(jnp.bfloat16),
        'w_dq': normal_weight(rng_keys[2], (D, Q_LORA), D),
        'g_q': jax.random.uniform(rng_keys[3], (Q_LORA,), jnp.float32, 0.5, 1.5).astype(jnp.bfloat16),
        'w_dkv': normal_weight(rng_keys[4], (D, KV_LORA + ROPE), D),
        'g_kv': jax.random.uniform(rng_keys[5], (KV_LORA,), jnp.float32, 0.5, 1.5).astype(jnp.bfloat16),
        'w_uq': normal_weight(rng_keys[6], (Q_LORA, HEADS, QK_DIM), Q_LORA),
        'w_uk': normal_weight(rng_keys[7], (KV_LORA, HEADS, NOPE), KV_LORA),
        'w_uv': normal_weight(rng_keys[8], (KV_LORA, HEADS, VHEAD), KV_LORA),
        'w_o': normal_weight(rng_keys[9], (HEADS, VHEAD, D), HEADS * VHEAD),
    }


def reference(hidden, grad_out, w_dq, g_q, w_dkv, g_kv, w_uq, w_uk, w_uv, w_o):
    attn_out, pullback = jax.vjp(forward, hidden, w_dq.astype(jnp.float32), g_q.astype(jnp.float32), w_dkv.astype(jnp.float32), g_kv.astype(jnp.float32), w_uq.astype(jnp.float32), w_uk.astype(jnp.float32), w_uv.astype(jnp.float32), w_o.astype(jnp.float32))
    all_grads = pullback(grad_out)
    return (attn_out, all_grads[0], all_grads[1], all_grads[2], all_grads[3], all_grads[4], all_grads[5], all_grads[6], all_grads[7], all_grads[8])
```

```python
import functools

import jax
import jax.numpy as jnp
from jax import lax
from jax.experimental import pallas as pl
from jax.experimental.pallas import tpu as pltpu
from jax.sharding import PartitionSpec as P

EPS = 1e-6
THETA = 10000.0
NEG_BIG = -1e30
LOG2E = 1.4426950408889634
F32 = jnp.float32
BF16 = jnp.bfloat16

NN = (((1,), (0,)), ((), ()))
NT = (((1,), (1,)), ((), ()))


def mm(a, b, dims=NN):
    return lax.dot_general(a, b, dims, preferred_element_type=F32)


def rope_tables(positions, rope_dim):
    inv_freq = 1.0 / (THETA ** (jnp.arange(rope_dim // 2, dtype=F32) * 2.0 / rope_dim))
    angles = positions.astype(F32)[:, None] * inv_freq[None, :]
    return jnp.cos(angles), jnp.sin(angles)


def apply_rope(values, cos_tab, sin_tab):
    half_dim = values.shape[-1] // 2
    lead_half = values[..., :half_dim]
    tail_half = values[..., half_dim:]
    return jnp.concatenate([lead_half * cos_tab - tail_half * sin_tab, tail_half * cos_tab + lead_half * sin_tab], axis=-1)


def unrope(grad_vals, cos_tab, sin_tab):
    half_dim = grad_vals.shape[-1] // 2
    lead_half = grad_vals[..., :half_dim]
    tail_half = grad_vals[..., half_dim:]
    return jnp.concatenate([lead_half * cos_tab + tail_half * sin_tab, tail_half * cos_tab - lead_half * sin_tab], axis=-1)


def norm_f32(raw_vals, gain_vec):
    inv_rms = lax.rsqrt(jnp.mean(raw_vals * raw_vals, axis=-1, keepdims=True) + EPS)
    return raw_vals * inv_rms * gain_vec


def attn_kernel(first, blk, scale, *refs):
    (rank_ref, qn_ref, qp_ref, do_ref, ckv_ref, ckvt_ref, kpe_ref, kpet_ref, wuk_ref, wuv_ref, cos_ref, sin_ref) = refs[:12]
    refs = refs[12:]
    if not first:
        dwk_in, dwv_in = refs[:2]
        refs = refs[6:]
    (o_ref, dqn_ref, dqp_ref, dc_ref, dkp_ref, dwk_ref, dwv_ref,
     k_s, kt_s, v_s, vt_s, e_s, g_s, p_s, ds_s, qm_s, dom_s, dk_s, dv_s) = refs
    step = pl.program_id(0)
    nkeys = ckv_ref.shape[1]
    qrows = qn_ref.shape[1]
    nope = 64
    lane128 = lax.broadcasted_iota(jnp.int32, (1, 128), 1)
    lane256 = lax.broadcasted_iota(jnp.int32, (1, 256), 1)
    coef = scale * LOG2E

    ckv = ckv_ref[0]
    ckvt = ckvt_ref[0]
    wuk = wuk_ref[...]
    wuv = wuv_ref[...]
    k_s[:, :256] = mm(ckv, wuk, NT).astype(BF16)
    v_s[...] = mm(ckv, wuv, NT).astype(BF16)
    kt_s[...] = mm(wuk, ckvt).astype(BF16)
    vt_s[...] = mm(wuv, ckvt).astype(BF16)

    def swap(u):
        return jnp.where(lane128 % 32 < 16, pltpu.roll(u, 112, 1), pltpu.roll(u, 16, 1))

    qpu = qp_ref[0].astype(F32)
    cos = cos_ref[...]
    sin = sin_ref[...]
    qpr = (qpu * cos + swap(qpu) * sin).astype(BF16)
    qn = qn_ref[0]
    do = do_ref[0]
    zero = jnp.zeros((), BF16)
    for h in range(4):
        pair = h // 2
        sel = (lane128 >= 64 * (h % 2)) & (lane128 < 64 * (h % 2) + 64)
        qm_s[h, :, :128] = jnp.where(sel, qn[:, pair * 128:pair * 128 + 128], zero)
        selp = (lane128 >= 32 * h) & (lane128 < 32 * h + 32)
        qm_s[h, :, 128:] = jnp.where(selp, qpr, zero)
        selo = (lane256 >= 64 * h) & (lane256 < 64 * h + 64)
        dom_s[h] = jnp.where(selo, do, zero)

    def one_block(row0, nk, add):
        rows = slice(row0, row0 + blk)
        nch = nk // blk
        dqp_parts = []
        for pair in range(2):
            kops = [jnp.concatenate([k_s[c * blk:(c + 1) * blk, pair * 128:pair * 128 + 128], kpe_ref[0, c * blk:(c + 1) * blk, :]], axis=1) for c in range(nch)]
            o_parts = []
            dq_parts = []
            for hh in range(2):
                h = 2 * pair + hh
                slot = h % 2
                qm = qm_s[h, rows, :]
                dom = dom_s[h, rows, :]
                mx = None
                for c in range(nch):
                    st = mm(kops[c], qm, NT)
                    if c == nch - 1:
                        keep = lax.broadcasted_iota(jnp.int32, (blk, blk), 0) <= lax.broadcasted_iota(jnp.int32, (blk, blk), 1)
                        st = jnp.where(keep, st, NEG_BIG)
                    e_s[slot, c * blk:(c + 1) * blk, :] = st
                    cm = jnp.max(st.reshape(blk // 8, 8, blk), axis=0)
                    mx = cm if mx is None else jnp.maximum(mx, cm)
                mx = jnp.max(mx, axis=0, keepdims=True)
                tot = None
                for c in range(nch):
                    ks = slice(c * blk, (c + 1) * blk)
                    e = jnp.exp2((e_s[slot, ks, :] - mx) * coef)
                    e_s[slot, ks, :] = e
                    dp = mm(v_s[ks, :], dom, NT)
                    g_s[slot, ks, :] = dp
                    ce = jnp.sum(e.reshape(blk // 8, 8, blk), axis=0)
                    cd = jnp.sum((e * dp).reshape(blk // 8, 8, blk), axis=0)
                    tot = (ce, cd) if tot is None else (tot[0] + ce, tot[1] + cd)
                inv = 1.0 / jnp.sum(tot[0], axis=0, keepdims=True)
                dot = jnp.sum(tot[1], axis=0, keepdims=True) * inv
                cols = slice(h * blk, (h + 1) * blk)
                for c in range(nch):
                    ks = slice(c * blk, (c + 1) * blk)
                    p = e_s[slot, ks, :] * inv
                    p_s[ks, cols] = p.astype(BF16)
                    ds_s[ks, cols] = (p * (g_s[slot, ks, :] - dot)).astype(BF16)
                hr = slice(h * nope, (h + 1) * nope)
                o_parts.append(mm(vt_s[hr, :nk], p_s[:nk, cols]))
                dqt = mm(jnp.concatenate([kt_s[hr, :nk], kpet_ref[0, :, :nk]], axis=0), ds_s[:nk, cols])
                dq_parts.append(dqt[:nope])
                dqp_parts.append(dqt[nope:])
            lanes = slice(pair * 128, pair * 128 + 128)
            o_ref[0, rows, lanes] = jnp.concatenate(o_parts, axis=0).T.astype(BF16)
            dqn_ref[0, rows, lanes] = (jnp.concatenate(dq_parts, axis=0).T * scale).astype(BF16)
            qcat = jnp.concatenate([qm_s[2 * pair, rows, :], qm_s[2 * pair + 1, rows, :]], axis=0)
            for c in range(nch):
                ks = slice(c * blk, (c + 1) * blk)
                dk = mm(ds_s[ks, pair * 2 * blk:(pair + 1) * 2 * blk], qcat)
                if add:
                    dk_s[pair, ks, :] += dk
                else:
                    dk_s[pair, ks, :] = dk
        dqp = jnp.concatenate(dqp_parts, axis=0).T * scale
        dqp_ref[0, rows, :] = (dqp * cos[rows] - swap(dqp) * sin[rows]).astype(BF16)
        docat = jnp.concatenate([dom_s[h, rows, :] for h in range(4)], axis=0)
        for c in range(nch):
            ks = slice(c * blk, (c + 1) * blk)
            dv = mm(p_s[ks, :], docat)
            if add:
                dv_s[ks, :] += dv
            else:
                dv_s[ks, :] = dv

    rank = rank_ref[0]
    hi = qrows - blk

    @pl.when(rank == 0)
    def _():
        one_block(hi, 4 * blk, False)
        one_block(0, blk, True)

    @pl.when(rank == 1)
    def _():
        one_block(hi, 3 * blk, False)
        dk_s[:, 3 * blk:, :] = jnp.zeros_like(dk_s[:, 3 * blk:, :])
        dv_s[3 * blk:, :] = jnp.zeros_like(dv_s[3 * blk:, :])
        one_block(0, 2 * blk, True)

    dkb = (jnp.concatenate([dk_s[0, :, :128], dk_s[1, :, :128]], axis=1) * scale).astype(BF16)
    dvb = dv_s[...].astype(BF16)
    dkp = (dk_s[0, :, 128:] + dk_s[1, :, 128:]) * scale
    dc = mm(dkb, wuk) + mm(dvb, wuv)
    dwk = mm(ckvt, dkb)
    dwv = mm(ckvt, dvb)
    if first:
        dwk_ref[...] = dwk
        dwv_ref[...] = dwv
    else:
        dwk_ref[...] = dwk_in[...] + dwk
        dwv_ref[...] = dwv_in[...] + dwv

    @pl.when(step == 0)
    def _():
        dc_ref[0] = dc
        dkp_ref[0] = dkp

    @pl.when(step > 0)
    def _():
        dc_ref[0] += dc
        dkp_ref[0] += dkp


def attention(j, rank_arr, qn, qp, do, ckv, ckvt, kpe4, kpet, wuk, wuv, cos, sin, prev, scale):
    nb, qrows, width = qn.shape
    nkeys, latent = ckv.shape[1:]
    groups = width // 256
    blk = qrows // 2
    first = prev is None
    row = lambda i: (j, 0, i)
    whole = lambda i: (j, 0, 0)
    in_specs = [
        pl.BlockSpec(memory_space=pltpu.SMEM),
        pl.BlockSpec((1, qrows, 256), row),
        pl.BlockSpec((1, qrows, 128), row),
        pl.BlockSpec((1, qrows, 256), row),
        pl.BlockSpec((1, nkeys, latent), whole),
        pl.BlockSpec((1, latent, nkeys), whole),
        pl.BlockSpec((1, nkeys, 128), whole),
        pl.BlockSpec((1, 32, nkeys), whole),
        pl.BlockSpec((256, latent), lambda i: (i, 0)),
        pl.BlockSpec((256, latent), lambda i: (i, 0)),
        pl.BlockSpec((qrows, 128), lambda i: (0, 0)),
        pl.BlockSpec((qrows, 128), lambda i: (0, 0)),
    ]
    args = [rank_arr, qn, qp, do, ckv, ckvt, kpe4, kpet, wuk, wuv, cos, sin]
    aliases = {}
    if not first:
        dqn, dqp, dc, dkp, dwk, dwv = prev
        in_specs += [pl.BlockSpec((latent, 256), lambda i: (0, i))] * 2 + [pl.BlockSpec(memory_space=pl.ANY)] * 4
        args += [dwk, dwv, dqn, dqp, dc, dkp]
        aliases = {12: 5, 13: 6, 14: 1, 15: 2, 16: 3, 17: 4}
    out_specs = [
        pl.BlockSpec((1, qrows, 256), lambda i: (0, 0, i)),
        pl.BlockSpec((1, qrows, 256), row),
        pl.BlockSpec((1, qrows, 128), row),
        pl.BlockSpec((1, nkeys, latent), whole),
        pl.BlockSpec((1, nkeys, 128), whole),
        pl.BlockSpec((latent, 256), lambda i: (0, i)),
        pl.BlockSpec((latent, 256), lambda i: (0, i)),
    ]
    out_shape = [
        jax.ShapeDtypeStruct((1, qrows, width), BF16),
        jax.ShapeDtypeStruct((nb, qrows, width), BF16),
        jax.ShapeDtypeStruct((nb, qrows, width // 2), BF16),
        jax.ShapeDtypeStruct((nb, nkeys, latent), F32),
        jax.ShapeDtypeStruct((nb, nkeys, 128), F32),
        jax.ShapeDtypeStruct((latent, width), F32),
        jax.ShapeDtypeStruct((latent, width), F32),
    ]
    scratch = [
        pltpu.VMEM((nkeys, 256), BF16), pltpu.VMEM((256, nkeys), BF16),
        pltpu.VMEM((nkeys, 256), BF16), pltpu.VMEM((256, nkeys), BF16),
        pltpu.VMEM((2, nkeys, blk), F32), pltpu.VMEM((2, nkeys, blk), F32),
        pltpu.VMEM((nkeys, 4 * blk), BF16), pltpu.VMEM((nkeys, 4 * blk), BF16),
        pltpu.VMEM((4, qrows, 256), BF16), pltpu.VMEM((4, qrows, 256), BF16),
        pltpu.VMEM((2, nkeys, 256), F32), pltpu.VMEM((nkeys, 256), F32),
    ]
    pairs = 5 * 4 * groups * blk * blk
    return pl.pallas_call(
        functools.partial(attn_kernel, first, blk, scale),
        grid=(groups,),
        in_specs=in_specs,
        out_specs=out_specs,
        out_shape=out_shape,
        scratch_shapes=scratch,
        input_output_aliases=aliases,
        name="attn_fwd_bwd",
        compiler_params=pltpu.CompilerParams(dimension_semantics=("arbitrary",), vmem_limit_bytes=56 * 1024 * 1024),
        cost_estimate=pl.CostEstimate(flops=pairs * 6 * 2 * 256, bytes_accessed=40 * 1024 * 1024, transcendentals=pairs),
    )(*args)


def out_kernel(o_ref, w_ref, *rest):
    y_ref = rest[-1]
    w = w_ref[...]
    for t in range(o_ref.shape[0]):
        y_ref[t, 0] = mm(o_ref[t], w).astype(BF16)


def out_proj(j, nb, o_all, w_o, prev):
    tp, rows, width = o_all.shape
    dim = w_o.shape[1]
    in_specs = [pl.BlockSpec((tp, rows, width), lambda i: (0, 0, 0)), pl.BlockSpec((width, 256), lambda i: (0, i))]
    args = [o_all, w_o]
    aliases = {}
    if prev is not None:
        in_specs.append(pl.BlockSpec(memory_space=pl.ANY))
        args.append(prev)
        aliases = {2: 0}
    return pl.pallas_call(
        out_kernel,
        grid=(dim // 256,),
        in_specs=in_specs,
        out_specs=pl.BlockSpec((tp, 1, rows, 256), lambda i: (0, j, 0, i)),
        out_shape=jax.ShapeDtypeStruct((tp, nb, rows, dim), BF16),
        input_output_aliases=aliases,
        name="out_proj",
        compiler_params=pltpu.CompilerParams(dimension_semantics=("arbitrary",), vmem_limit_bytes=56 * 1024 * 1024),
        cost_estimate=pl.CostEstimate(flops=2 * tp * rows * width * dim, bytes_accessed=2 * (2 * tp * rows * width + width * dim), transcendentals=0),
    )(*args)


def solution(mesh):
    cp_size = mesh.shape['cp']
    tp_size = mesh.shape['tp']
    swap_pairs = [(0, 1), (1, 0)]

    def per_device(hidden, grad_out, w_dq, g_q, w_dkv, g_kv, w_uq, w_uk, w_uv, w_o):
        cp_rank = lax.axis_index('cp')
        tp_rank = lax.axis_index('tp')
        n_batch, seq_local, dim = hidden.shape
        nb = n_batch // tp_size
        q_lora = w_dq.shape[1]
        kv_lora = g_kv.shape[0]
        nope = w_uk.shape[2]
        qk_dim = w_uq.shape[2]
        rope_dim = qk_dim - nope
        heads_dev = w_uq.shape[1]
        heads = heads_dev * tp_size
        v_dim = w_uv.shape[2]
        scale = qk_dim ** -0.5
        half_len = seq_local // 2
        half_heads = heads_dev // 2

        def gather_weight(w):
            half = lax.dynamic_slice_in_dim(w, cp_rank * half_heads, half_heads, 0)
            return lax.all_gather(half, ('tp', 'cp'), axis=0, tiled=True)

        wq_all = gather_weight(jnp.transpose(w_uq, (1, 2, 0)))
        wkv_all = gather_weight(jnp.concatenate([jnp.transpose(w_uk, (1, 2, 0)), jnp.transpose(w_uv, (1, 2, 0))], axis=1))
        wo_all = gather_weight(w_o).reshape(heads * v_dim, dim)
        wqn = wq_all[:, :nope].reshape(heads * nope, q_lora)
        wqp = wq_all[:, nope:].reshape(heads * rope_dim, q_lora)
        wuk = wkv_all[:, :nope].reshape(heads * nope, kv_lora)
        wuv = wkv_all[:, nope:].reshape(heads * v_dim, kv_lora)

        local_idx = jnp.arange(seq_local, dtype=jnp.int32)
        block_id = jnp.where(local_idx < half_len, cp_rank, 2 * cp_size - 1 - cp_rank)
        positions = block_id * half_len + local_idx % half_len
        cos_tab, sin_tab = rope_tables(positions, rope_dim)
        cos128 = jnp.tile(cos_tab, (1, 8))
        sin128 = jnp.tile(jnp.concatenate([-sin_tab, sin_tab], axis=1), (1, 4))

        w_cat = jnp.concatenate([w_dq, w_dkv], axis=1)
        x_own = lax.dynamic_slice_in_dim(hidden, tp_rank * nb, nb, 0)
        dy_own = lax.dynamic_slice_in_dim(grad_out, tp_rank * nb, nb, 0)

        raw = jnp.einsum('btd,dq->btq', x_own, w_cat, preferred_element_type=F32).astype(BF16)
        cq_f32 = raw[..., :q_lora].astype(F32)
        ckv_f32 = raw[..., q_lora:q_lora + kv_lora].astype(F32)
        gq_f32 = g_q.astype(F32)
        gkv_f32 = g_kv.astype(F32)
        c_q = norm_f32(cq_f32, gq_f32).astype(BF16)
        c_kv = norm_f32(ckv_f32, gkv_f32).astype(BF16)
        k_pe = apply_rope(raw[..., q_lora + kv_lora:].astype(F32), cos_tab, sin_tab).astype(BF16)

        def by_position(own, other):
            lo = jnp.where(cp_rank == 0, own[:, :half_len], other[:, :half_len])
            lo2 = jnp.where(cp_rank == 0, other[:, :half_len], own[:, :half_len])
            hi = jnp.where(cp_rank == 0, other[:, half_len:], own[:, half_len:])
            hi2 = jnp.where(cp_rank == 0, own[:, half_len:], other[:, half_len:])
            return jnp.concatenate([lo, lo2, hi, hi2], axis=1)

        other_kv, other_pe = lax.ppermute((c_kv, k_pe), 'cp', swap_pairs)
        ckv_seq = by_position(c_kv, other_kv)
        kpe_seq = by_position(k_pe, other_pe)
        ckvt_seq = jnp.swapaxes(ckv_seq, 1, 2)
        kpet_seq = jnp.swapaxes(kpe_seq, 1, 2)
        kpe4 = jnp.tile(kpe_seq, (1, 1, 4))

        qn = jnp.einsum('btq,fq->btf', c_q, wqn, preferred_element_type=F32).astype(BF16)
        qp = jnp.einsum('btq,fq->btf', c_q, wqp, preferred_element_type=F32).astype(BF16)
        grad_o = jnp.einsum('btd,fd->btf', dy_own, wo_all, preferred_element_type=F32).astype(BF16)

        rank_arr = cp_rank.astype(jnp.int32).reshape(1)
        prev = None
        o_all = []
        for j in range(nb):
            res = attention(j, rank_arr, qn, qp, grad_o, ckv_seq, ckvt_seq, kpe4, kpet_seq, wuk, wuv, cos128, sin128, prev, scale)
            o_all.append(lax.all_gather(res[0], 'tp', axis=0, tiled=True))
            prev = res[1:]
        dqn, dqp, dc_seq, dkp_seq, dwk, dwv = prev

        dkp_seq = dkp_seq[..., :32] + dkp_seq[..., 32:64] + dkp_seq[..., 64:96] + dkp_seq[..., 96:]
        lat = jnp.concatenate([dc_seq, dkp_seq], axis=-1)
        b0, b1, b2, b3 = (lat[:, i * half_len:(i + 1) * half_len] for i in range(4))
        outer = jnp.concatenate([b0, b3], axis=1)
        inner = jnp.concatenate([b1, b2], axis=1)
        mine = jnp.where(cp_rank == 0, outer, inner)
        theirs = jnp.where(cp_rank == 0, inner, outer)
        lat = mine + lax.ppermute(theirs, 'cp', swap_pairs)
        grad_cq = jnp.einsum('btf,fq->btq', dqn, wqn, preferred_element_type=F32) + jnp.einsum('btf,fq->btq', dqp, wqp, preferred_element_type=F32)

        norm_q_pull = jax.vjp(norm_f32, cq_f32, gq_f32)[1]
        grad_cq_raw, grad_g_q = norm_q_pull(grad_cq)
        norm_kv_pull = jax.vjp(norm_f32, ckv_f32, gkv_f32)[1]
        grad_ckv_raw, grad_g_kv = norm_kv_pull(lat[..., :kv_lora])
        grad_raw = jnp.concatenate([grad_cq_raw, grad_ckv_raw, unrope(lat[..., kv_lora:], cos_tab, sin_tab)], axis=-1).astype(BF16)
        grad_raw = lax.all_gather(grad_raw, 'tp', axis=0, tiled=True)
        grad_g = lax.psum(jnp.concatenate([grad_g_q, grad_g_kv]), ('tp', 'cp'))

        q_half = q_lora // 2
        cq_mine = lax.dynamic_slice_in_dim(c_q, cp_rank * q_half, q_half, 2)
        cq_theirs = lax.dynamic_slice_in_dim(c_q, (1 - cp_rank) * q_half, q_half, 2)

        def dw_of(dq, cq):
            return jnp.einsum('btf,btq->fq', dq, cq, preferred_element_type=F32)

        dwqn = dw_of(dqn, cq_mine) + lax.ppermute(dw_of(dqn, cq_theirs), 'cp', swap_pairs)
        dwqp = dw_of(dqp, cq_mine) + lax.ppermute(dw_of(dqp, cq_theirs), 'cp', swap_pairs)
        c_half = kv_lora // 2
        dw_kv = jnp.stack([dwk, dwv])
        kv_mine = lax.dynamic_slice_in_dim(dw_kv, cp_rank * c_half, c_half, 1)
        kv_theirs = lax.dynamic_slice_in_dim(dw_kv, (1 - cp_rank) * c_half, c_half, 1)
        dw_kv = kv_mine + lax.ppermute(kv_theirs, 'cp', swap_pairs)
        dwqn = lax.psum_scatter(dwqn, 'tp', scatter_dimension=0, tiled=True)
        dwqp = lax.psum_scatter(dwqp, 'tp', scatter_dimension=0, tiled=True)
        dw_kv = lax.psum_scatter(dw_kv, 'tp', scatter_dimension=2, tiled=True)
        dwq = jnp.concatenate([dwqn.reshape(heads_dev, nope, q_half), dwqp.reshape(heads_dev, rope_dim, q_half)], axis=1)

        def join(part, axis):
            other = lax.ppermute(part, 'cp', swap_pairs)
            return jnp.concatenate([jnp.where(cp_rank == 0, part, other), jnp.where(cp_rank == 0, other, part)], axis=axis)

        grad_w_uq = jnp.transpose(join(dwq, 2), (2, 0, 1))
        dw_kv = join(dw_kv, 1)
        grad_w_uk = dw_kv[0].reshape(kv_lora, heads_dev, nope)
        grad_w_uv = dw_kv[1].reshape(kv_lora, heads_dev, v_dim)

        y = None
        for j in range(nb):
            y = out_proj(j, nb, o_all[j], wo_all, y)
        attn_out = y.reshape(n_batch, seq_local, dim)
        cols = heads_dev * v_dim
        o_mine = jnp.stack([lax.dynamic_slice_in_dim(o, tp_rank * cols, cols, 2) for o in o_all], axis=1).reshape(n_batch, seq_local, cols)
        dwo = jnp.einsum('btf,btd->fd', o_mine, grad_out, preferred_element_type=F32)
        grad_w_o = (dwo + lax.ppermute(dwo, 'cp', swap_pairs)).reshape(heads_dev, v_dim, dim)

        dw_cat = jnp.einsum('btd,btq->dq', hidden, grad_raw, preferred_element_type=F32)
        dw_other = lax.ppermute(dw_cat, 'cp', swap_pairs)
        grad_w_dq = dw_cat[:, :q_lora] + dw_other[:, :q_lora]
        grad_w_dkv = dw_cat[:, q_lora:] + dw_other[:, q_lora:]
        grad_hidden = jnp.einsum('btq,dq->btd', grad_raw, w_cat, preferred_element_type=F32).astype(BF16)
        return (attn_out, grad_hidden, grad_w_dq, grad_g[:q_lora], grad_w_dkv, grad_g[q_lora:], grad_w_uq, grad_w_uk, grad_w_uv, grad_w_o)

    seq_spec = P(None, 'cp', None)
    full_spec = P()
    head_spec = P(None, 'tp', None)
    out_head_spec = P('tp', None, None)
    all_specs = (seq_spec, seq_spec, full_spec, full_spec, full_spec, full_spec, head_spec, head_spec, head_spec, out_head_spec)
    return jax.shard_map(per_device, mesh=mesh, in_specs=all_specs, out_specs=all_specs, check_vma=False)
```

```python
import functools

import jax
import jax.numpy as jnp
from jax import lax
from jax.experimental import pallas as pl
from jax.experimental.pallas import tpu as pltpu
from jax.sharding import PartitionSpec as P


EPS = 1e-6
THETA = 10000.0
NEG_BIG = -1e30
LOG2E = 1.4426950408889634
F32 = jnp.float32
BF16 = jnp.bfloat16

NN = (((1,), (0,)), ((), ()))
NT = (((1,), (1,)), ((), ()))


def mm(a, b, dims=NN):
    return lax.dot_general(a, b, dims, preferred_element_type=F32)


def rope_tables(positions, rope_dim):
    inv_freq = 1.0 / (THETA ** (jnp.arange(rope_dim // 2, dtype=F32) * 2.0 / rope_dim))
    angles = positions.astype(F32)[:, None] * inv_freq[None, :]
    return jnp.cos(angles), jnp.sin(angles)


def apply_rope(values, cos_tab, sin_tab):
    half_dim = values.shape[-1] // 2
    lead_half = values[..., :half_dim]
    tail_half = values[..., half_dim:]
    return jnp.concatenate([lead_half * cos_tab - tail_half * sin_tab, tail_half * cos_tab + lead_half * sin_tab], axis=-1)


def unrope(grad_vals, cos_tab, sin_tab):
    half_dim = grad_vals.shape[-1] // 2
    lead_half = grad_vals[..., :half_dim]
    tail_half = grad_vals[..., half_dim:]
    return jnp.concatenate([lead_half * cos_tab + tail_half * sin_tab, tail_half * cos_tab - lead_half * sin_tab], axis=-1)


def norm_f32(raw_vals, gain_vec):
    inv_rms = lax.rsqrt(jnp.mean(raw_vals * raw_vals, axis=-1, keepdims=True) + EPS)
    return raw_vals * inv_rms * gain_vec


def attn_kernel(first, blk, scale, *refs):
    (rank_ref, qn_ref, qp_ref, do_ref, ckv_ref, ckvt_ref, kpe_ref, kpet_ref, wuk_ref, wuv_ref, cos_ref, sin_ref) = refs[:12]
    refs = refs[12:]
    if not first:
        dwk_in, dwv_in = refs[:2]
        refs = refs[6:]
    (o_ref, dqn_ref, dqp_ref, dc_ref, dkp_ref, dwk_ref, dwv_ref,
     k_s, kt_s, v_s, vt_s, e_s, g_s, p_s, ds_s, qm_s, dom_s, dk_s, dv_s) = refs
    step = pl.program_id(0)
    qrows = qn_ref.shape[1]
    nope = 64
    lane128 = lax.broadcasted_iota(jnp.int32, (1, 128), 1)
    lane256 = lax.broadcasted_iota(jnp.int32, (1, 256), 1)
    coef = scale * LOG2E

    ckv = ckv_ref[0]
    ckvt = ckvt_ref[0]
    wuk = wuk_ref[...]
    wuv = wuv_ref[...]
    k_s[:, :256] = mm(ckv, wuk, NT).astype(BF16)
    v_s[...] = mm(ckv, wuv, NT).astype(BF16)
    kt_s[...] = mm(wuk, ckvt).astype(BF16)
    vt_s[...] = mm(wuv, ckvt).astype(BF16)

    def swap(u):
        return jnp.where(lane128 % 32 < 16, pltpu.roll(u, 112, 1), pltpu.roll(u, 16, 1))

    qpu = qp_ref[0].astype(F32)
    cos = cos_ref[...]
    sin = sin_ref[...]
    qpr = (qpu * cos + swap(qpu) * sin).astype(BF16)
    qn = qn_ref[0]
    do = do_ref[0]
    zero = jnp.zeros((), BF16)
    for h in range(4):
        pair = h // 2
        sel = (lane128 >= 64 * (h % 2)) & (lane128 < 64 * (h % 2) + 64)
        qm_s[h, :, :128] = jnp.where(sel, qn[:, pair * 128:pair * 128 + 128], zero)
        selp = (lane128 >= 32 * h) & (lane128 < 32 * h + 32)
        qm_s[h, :, 128:] = jnp.where(selp, qpr, zero)
        selo = (lane256 >= 64 * h) & (lane256 < 64 * h + 64)
        dom_s[h] = jnp.where(selo, do, zero)

    def one_block(row0, nk, add):
        rows = slice(row0, row0 + blk)
        nch = nk // blk
        dqp_parts = []
        for pair in range(2):
            kops = [jnp.concatenate([k_s[c * blk:(c + 1) * blk, pair * 128:pair * 128 + 128], kpe_ref[0, c * blk:(c + 1) * blk, :]], axis=1) for c in range(nch)]
            o_parts = []
            dq_parts = []
            for hh in range(2):
                h = 2 * pair + hh
                slot = h % 2
                qm = qm_s[h, rows, :]
                dom = dom_s[h, rows, :]
                mx = None
                for c in range(nch):
                    st = mm(kops[c], qm, NT)
                    if c == nch - 1:
                        keep = lax.broadcasted_iota(jnp.int32, (blk, blk), 0) <= lax.broadcasted_iota(jnp.int32, (blk, blk), 1)
                        st = jnp.where(keep, st, NEG_BIG)
                    e_s[slot, c * blk:(c + 1) * blk, :] = st
                    cm = jnp.max(st.reshape(blk // 8, 8, blk), axis=0)
                    mx = cm if mx is None else jnp.maximum(mx, cm)
                mx = jnp.max(mx, axis=0, keepdims=True)
                tot = None
                for c in range(nch):
                    ks = slice(c * blk, (c + 1) * blk)
                    e = jnp.exp2((e_s[slot, ks, :] - mx) * coef)
                    e_s[slot, ks, :] = e
                    dp = mm(v_s[ks, :], dom, NT)
                    g_s[slot, ks, :] = dp
                    ce = jnp.sum(e.reshape(blk // 8, 8, blk), axis=0)
                    cd = jnp.sum((e * dp).reshape(blk // 8, 8, blk), axis=0)
                    tot = (ce, cd) if tot is None else (tot[0] + ce, tot[1] + cd)
                inv = 1.0 / jnp.sum(tot[0], axis=0, keepdims=True)
                dot = jnp.sum(tot[1], axis=0, keepdims=True) * inv
                cols = slice(h * blk, (h + 1) * blk)
                for c in range(nch):
                    ks = slice(c * blk, (c + 1) * blk)
                    p = e_s[slot, ks, :] * inv
                    p_s[ks, cols] = p.astype(BF16)
                    ds_s[ks, cols] = (p * (g_s[slot, ks, :] - dot)).astype(BF16)
                hr = slice(h * nope, (h + 1) * nope)
                o_parts.append(mm(vt_s[hr, :nk], p_s[:nk, cols]))
                dqt = mm(jnp.concatenate([kt_s[hr, :nk], kpet_ref[0, :, :nk]], axis=0), ds_s[:nk, cols])
                dq_parts.append(dqt[:nope])
                dqp_parts.append(dqt[nope:])
            lanes = slice(pair * 128, pair * 128 + 128)
            o_ref[0, rows, lanes] = jnp.concatenate(o_parts, axis=0).T.astype(BF16)
            dqn_ref[0, rows, lanes] = (jnp.concatenate(dq_parts, axis=0).T * scale).astype(BF16)
            qcat = jnp.concatenate([qm_s[2 * pair, rows, :], qm_s[2 * pair + 1, rows, :]], axis=0)
            for c in range(nch):
                ks = slice(c * blk, (c + 1) * blk)
                dk = mm(ds_s[ks, pair * 2 * blk:(pair + 1) * 2 * blk], qcat)
                if add:
                    dk_s[pair, ks, :] += dk
                else:
                    dk_s[pair, ks, :] = dk
        dqp = jnp.concatenate(dqp_parts, axis=0).T * scale
        dqp_ref[0, rows, :] = (dqp * cos[rows] - swap(dqp) * sin[rows]).astype(BF16)
        docat = jnp.concatenate([dom_s[h, rows, :] for h in range(4)], axis=0)
        for c in range(nch):
            ks = slice(c * blk, (c + 1) * blk)
            dv = mm(p_s[ks, :], docat)
            if add:
                dv_s[ks, :] += dv
            else:
                dv_s[ks, :] = dv

    rank = rank_ref[0]
    hi = qrows - blk

    @pl.when(rank == 0)
    def _():
        one_block(hi, 4 * blk, False)
        one_block(0, blk, True)

    @pl.when(rank == 1)
    def _():
        one_block(hi, 3 * blk, False)
        dk_s[:, 3 * blk:, :] = jnp.zeros_like(dk_s[:, 3 * blk:, :])
        dv_s[3 * blk:, :] = jnp.zeros_like(dv_s[3 * blk:, :])
        one_block(0, 2 * blk, True)

    dkb = (jnp.concatenate([dk_s[0, :, :128], dk_s[1, :, :128]], axis=1) * scale).astype(BF16)
    dvb = dv_s[...].astype(BF16)
    dkp = (dk_s[0, :, 128:] + dk_s[1, :, 128:]) * scale
    dc = mm(dkb, wuk) + mm(dvb, wuv)
    dwk = mm(ckvt, dkb)
    dwv = mm(ckvt, dvb)
    if first:
        dwk_ref[...] = dwk
        dwv_ref[...] = dwv
    else:
        dwk_ref[...] = dwk_in[...] + dwk
        dwv_ref[...] = dwv_in[...] + dwv

    @pl.when(step == 0)
    def _():
        dc_ref[0] = dc
        dkp_ref[0] = dkp

    @pl.when(step > 0)
    def _():
        dc_ref[0] += dc
        dkp_ref[0] += dkp


def fwd_kernel(blk, scale, rank_ref, qn_ref, qp_ref, ckv_ref, ckvt_ref, kpe_ref, wuk_ref, wuv_ref, cos_ref, sin_ref, o_ref, k_s, vt_s, e_s, p_s, qm_s):
    lane128 = lax.broadcasted_iota(jnp.int32, (1, 128), 1)
    coef = scale * LOG2E
    qrows = qn_ref.shape[1]
    k_s[...] = mm(ckv_ref[0], wuk_ref[...], NT).astype(BF16)
    vt_s[...] = mm(wuv_ref[...], ckvt_ref[0]).astype(BF16)
    qpu = qp_ref[0].astype(F32)
    swapped = jnp.where(lane128 % 32 < 16, pltpu.roll(qpu, 112, 1), pltpu.roll(qpu, 16, 1))
    qpr = (qpu * cos_ref[...] + swapped * sin_ref[...]).astype(BF16)
    zero = jnp.zeros((), BF16)
    for h in range(4):
        pair = h // 2
        sel = (lane128 >= 64 * (h % 2)) & (lane128 < 64 * (h % 2) + 64)
        qm_s[h, :, :128] = jnp.where(sel, qn_ref[0, :, pair * 128:pair * 128 + 128], zero)
        selp = (lane128 >= 32 * h) & (lane128 < 32 * h + 32)
        qm_s[h, :, 128:] = jnp.where(selp, qpr, zero)

    def one_block(row0, nk):
        rows = slice(row0, row0 + blk)
        nch = nk // blk
        for pair in range(2):
            o_parts = []
            for hh in range(2):
                h = 2 * pair + hh
                slot = h % 2
                qm = qm_s[h, rows, :]
                mx = None
                for c in range(nch):
                    ks = slice(c * blk, (c + 1) * blk)
                    st = mm(jnp.concatenate([k_s[ks, pair * 128:pair * 128 + 128], kpe_ref[0, ks, :]], axis=1), qm, NT)
                    if c == nch - 1:
                        keep = lax.broadcasted_iota(jnp.int32, (blk, blk), 0) <= lax.broadcasted_iota(jnp.int32, (blk, blk), 1)
                        st = jnp.where(keep, st, NEG_BIG)
                    e_s[slot, ks, :] = st
                    cm = jnp.max(st.reshape(blk // 8, 8, blk), axis=0)
                    mx = cm if mx is None else jnp.maximum(mx, cm)
                mx = jnp.max(mx, axis=0, keepdims=True)
                tot = None
                for c in range(nch):
                    ks = slice(c * blk, (c + 1) * blk)
                    e = jnp.exp2((e_s[slot, ks, :] - mx) * coef)
                    e_s[slot, ks, :] = e
                    ce = jnp.sum(e.reshape(blk // 8, 8, blk), axis=0)
                    tot = ce if tot is None else tot + ce
                inv = 1.0 / jnp.sum(tot, axis=0, keepdims=True)
                for c in range(nch):
                    ks = slice(c * blk, (c + 1) * blk)
                    p_s[slot, ks, :] = (e_s[slot, ks, :] * inv).astype(BF16)
                o_parts.append(mm(vt_s[h * 64:(h + 1) * 64, :nk], p_s[slot, :nk, :]))
            o_ref[0, rows, pair * 128:pair * 128 + 128] = jnp.concatenate(o_parts, axis=0).T.astype(BF16)

    rank = rank_ref[0]

    @pl.when(rank == 0)
    def _():
        one_block(qrows - blk, 4 * blk)
        one_block(0, blk)

    @pl.when(rank == 1)
    def _():
        one_block(qrows - blk, 3 * blk)
        one_block(0, 2 * blk)


def attention_fwd(j, rank_arr, qn, qp, ckv, ckvt, kpe4, wuk, wuv, cos, sin, scale):
    _, qrows, width = qn.shape
    nkeys, latent = ckv.shape[1:]
    groups = width // 256
    blk = qrows // 2
    row = lambda i: (j, 0, i)
    whole = lambda i: (j, 0, 0)
    pairs = 5 * 4 * groups * blk * blk
    return pl.pallas_call(
        functools.partial(fwd_kernel, blk, scale),
        grid=(groups,),
        in_specs=[
            pl.BlockSpec(memory_space=pltpu.SMEM),
            pl.BlockSpec((1, qrows, 256), row),
            pl.BlockSpec((1, qrows, 128), row),
            pl.BlockSpec((1, nkeys, latent), whole),
            pl.BlockSpec((1, latent, nkeys), whole),
            pl.BlockSpec((1, nkeys, 128), whole),
            pl.BlockSpec((256, latent), lambda i: (i, 0)),
            pl.BlockSpec((256, latent), lambda i: (i, 0)),
            pl.BlockSpec((qrows, 128), lambda i: (0, 0)),
            pl.BlockSpec((qrows, 128), lambda i: (0, 0)),
        ],
        out_specs=pl.BlockSpec((1, qrows, 256), lambda i: (0, 0, i)),
        out_shape=jax.ShapeDtypeStruct((1, qrows, width), BF16),
        scratch_shapes=[
            pltpu.VMEM((nkeys, 256), BF16), pltpu.VMEM((256, nkeys), BF16),
            pltpu.VMEM((2, nkeys, blk), F32), pltpu.VMEM((2, nkeys, blk), BF16),
            pltpu.VMEM((4, qrows, 256), BF16),
        ],
        name="attn_fwd",
        compiler_params=pltpu.CompilerParams(dimension_semantics=("arbitrary",), vmem_limit_bytes=40 * 1024 * 1024),
        cost_estimate=pl.CostEstimate(flops=pairs * 2 * 2 * 256, bytes_accessed=10 * 1024 * 1024, transcendentals=pairs),
    )(rank_arr, qn, qp, ckv, ckvt, kpe4, wuk, wuv, cos, sin)


def attention(j, rank_arr, qn, qp, do, ckv, ckvt, kpe4, kpet, wuk, wuv, cos, sin, prev, scale):
    nb, qrows, width = qn.shape
    nkeys, latent = ckv.shape[1:]
    groups = width // 256
    blk = qrows // 2
    first = prev is None
    row = lambda i: (j, 0, i)
    whole = lambda i: (j, 0, 0)
    in_specs = [
        pl.BlockSpec(memory_space=pltpu.SMEM),
        pl.BlockSpec((1, qrows, 256), row),
        pl.BlockSpec((1, qrows, 128), row),
        pl.BlockSpec((1, qrows, 256), row),
        pl.BlockSpec((1, nkeys, latent), whole),
        pl.BlockSpec((1, latent, nkeys), whole),
        pl.BlockSpec((1, nkeys, 128), whole),
        pl.BlockSpec((1, 32, nkeys), whole),
        pl.BlockSpec((256, latent), lambda i: (i, 0)),
        pl.BlockSpec((256, latent), lambda i: (i, 0)),
        pl.BlockSpec((qrows, 128), lambda i: (0, 0)),
        pl.BlockSpec((qrows, 128), lambda i: (0, 0)),
    ]
    args = [rank_arr, qn, qp, do, ckv, ckvt, kpe4, kpet, wuk, wuv, cos, sin]
    aliases = {}
    if not first:
        dqn, dqp, dc, dkp, dwk, dwv = prev
        in_specs += [pl.BlockSpec((latent, 256), lambda i: (0, i))] * 2 + [pl.BlockSpec(memory_space=pl.ANY)] * 4
        args += [dwk, dwv, dqn, dqp, dc, dkp]
        aliases = {12: 5, 13: 6, 14: 1, 15: 2, 16: 3, 17: 4}
    out_specs = [
        pl.BlockSpec((1, qrows, 256), lambda i: (0, 0, i)),
        pl.BlockSpec((1, qrows, 256), row),
        pl.BlockSpec((1, qrows, 128), row),
        pl.BlockSpec((1, nkeys, latent), whole),
        pl.BlockSpec((1, nkeys, 128), whole),
        pl.BlockSpec((latent, 256), lambda i: (0, i)),
        pl.BlockSpec((latent, 256), lambda i: (0, i)),
    ]
    out_shape = [
        jax.ShapeDtypeStruct((1, qrows, width), BF16),
        jax.ShapeDtypeStruct((nb, qrows, width), BF16),
        jax.ShapeDtypeStruct((nb, qrows, width // 2), BF16),
        jax.ShapeDtypeStruct((nb, nkeys, latent), F32),
        jax.ShapeDtypeStruct((nb, nkeys, 128), F32),
        jax.ShapeDtypeStruct((latent, width), F32),
        jax.ShapeDtypeStruct((latent, width), F32),
    ]
    scratch = [
        pltpu.VMEM((nkeys, 256), BF16), pltpu.VMEM((256, nkeys), BF16),
        pltpu.VMEM((nkeys, 256), BF16), pltpu.VMEM((256, nkeys), BF16),
        pltpu.VMEM((2, nkeys, blk), F32), pltpu.VMEM((2, nkeys, blk), F32),
        pltpu.VMEM((nkeys, 4 * blk), BF16), pltpu.VMEM((nkeys, 4 * blk), BF16),
        pltpu.VMEM((4, qrows, 256), BF16), pltpu.VMEM((4, qrows, 256), BF16),
        pltpu.VMEM((2, nkeys, 256), F32), pltpu.VMEM((nkeys, 256), F32),
    ]
    pairs = 5 * 4 * groups * blk * blk
    return pl.pallas_call(
        functools.partial(attn_kernel, first, blk, scale),
        grid=(groups,),
        in_specs=in_specs,
        out_specs=out_specs,
        out_shape=out_shape,
        scratch_shapes=scratch,
        input_output_aliases=aliases,
        name="attn_fwd_bwd",
        compiler_params=pltpu.CompilerParams(dimension_semantics=("arbitrary",), vmem_limit_bytes=56 * 1024 * 1024),
        cost_estimate=pl.CostEstimate(flops=pairs * 6 * 2 * 256, bytes_accessed=40 * 1024 * 1024, transcendentals=pairs),
    )(*args)


def out_kernel(o_ref, w_ref, *rest):
    y_ref = rest[-1]
    w = w_ref[...]
    for t in range(o_ref.shape[0]):
        y_ref[t, 0] = mm(o_ref[t], w).astype(BF16)


def out_proj(j, nb, o_all, w_o, prev):
    tp, rows, width = o_all.shape
    dim = w_o.shape[1]
    in_specs = [pl.BlockSpec((tp, rows, width), lambda i: (0, 0, 0)), pl.BlockSpec((width, 256), lambda i: (0, i))]
    args = [o_all, w_o]
    aliases = {}
    if prev is not None:
        in_specs.append(pl.BlockSpec(memory_space=pl.ANY))
        args.append(prev)
        aliases = {2: 0}
    return pl.pallas_call(
        out_kernel,
        grid=(dim // 256,),
        in_specs=in_specs,
        out_specs=pl.BlockSpec((tp, 1, rows, 256), lambda i: (0, j, 0, i)),
        out_shape=jax.ShapeDtypeStruct((tp, nb, rows, dim), BF16),
        input_output_aliases=aliases,
        name="out_proj",
        compiler_params=pltpu.CompilerParams(dimension_semantics=("arbitrary",), vmem_limit_bytes=56 * 1024 * 1024),
        cost_estimate=pl.CostEstimate(flops=2 * tp * rows * width * dim, bytes_accessed=2 * (2 * tp * rows * width + width * dim), transcendentals=0),
    )(*args)


def solution(mesh):
    cp_size = mesh.shape['cp']
    tp_size = mesh.shape['tp']
    swap_pairs = [(0, 1), (1, 0)]

    def per_device(hidden, grad_out, w_dq, g_q, w_dkv, g_kv, w_uq, w_uk, w_uv, w_o):
        cp_rank = lax.axis_index('cp')
        tp_rank = lax.axis_index('tp')
        n_batch, seq_local, dim = hidden.shape
        nb = n_batch // tp_size
        q_lora = w_dq.shape[1]
        kv_lora = g_kv.shape[0]
        nope = w_uk.shape[2]
        qk_dim = w_uq.shape[2]
        rope_dim = qk_dim - nope
        heads_dev = w_uq.shape[1]
        heads = heads_dev * tp_size
        v_dim = w_uv.shape[2]
        scale = qk_dim ** -0.5
        half_len = seq_local // 2
        half_heads = heads_dev // 2

        def gather_weight(w):
            half = lax.dynamic_slice_in_dim(w, cp_rank * half_heads, half_heads, 0)
            return lax.all_gather(half, ('tp', 'cp'), axis=0, tiled=True)

        wq_all = gather_weight(jnp.transpose(w_uq, (1, 2, 0)))
        wkv_all = gather_weight(jnp.concatenate([jnp.transpose(w_uk, (1, 2, 0)), jnp.transpose(w_uv, (1, 2, 0))], axis=1))
        wo_all = gather_weight(w_o).reshape(heads * v_dim, dim)
        wqn = wq_all[:, :nope].reshape(heads * nope, q_lora)
        wqp = wq_all[:, nope:].reshape(heads * rope_dim, q_lora)
        wuk = wkv_all[:, :nope].reshape(heads * nope, kv_lora)
        wuv = wkv_all[:, nope:].reshape(heads * v_dim, kv_lora)

        local_idx = jnp.arange(seq_local, dtype=jnp.int32)
        block_id = jnp.where(local_idx < half_len, cp_rank, 2 * cp_size - 1 - cp_rank)
        positions = block_id * half_len + local_idx % half_len
        cos_tab, sin_tab = rope_tables(positions, rope_dim)
        cos128 = jnp.tile(cos_tab, (1, 8))
        sin128 = jnp.tile(jnp.concatenate([-sin_tab, sin_tab], axis=1), (1, 4))

        w_cat = jnp.concatenate([w_dq, w_dkv], axis=1)
        x_own = lax.dynamic_slice_in_dim(hidden, tp_rank * nb, nb, 0)
        dy_own = lax.dynamic_slice_in_dim(grad_out, tp_rank * nb, nb, 0)

        raw = jnp.einsum('btd,dq->btq', x_own, w_cat, preferred_element_type=F32).astype(BF16)
        cq_f32 = raw[..., :q_lora].astype(F32)
        ckv_f32 = raw[..., q_lora:q_lora + kv_lora].astype(F32)
        gq_f32 = g_q.astype(F32)
        gkv_f32 = g_kv.astype(F32)
        c_q = norm_f32(cq_f32, gq_f32).astype(BF16)
        c_kv = norm_f32(ckv_f32, gkv_f32).astype(BF16)
        k_pe = apply_rope(raw[..., q_lora + kv_lora:].astype(F32), cos_tab, sin_tab).astype(BF16)

        def by_position(own, other):
            lo = jnp.where(cp_rank == 0, own[:, :half_len], other[:, :half_len])
            lo2 = jnp.where(cp_rank == 0, other[:, :half_len], own[:, :half_len])
            hi = jnp.where(cp_rank == 0, other[:, half_len:], own[:, half_len:])
            hi2 = jnp.where(cp_rank == 0, own[:, half_len:], other[:, half_len:])
            return jnp.concatenate([lo, lo2, hi, hi2], axis=1)

        other_kv, other_pe = lax.ppermute((c_kv, k_pe), 'cp', swap_pairs)
        ckv_seq = by_position(c_kv, other_kv)
        kpe_seq = by_position(k_pe, other_pe)
        ckvt_seq = jnp.swapaxes(ckv_seq, 1, 2)
        kpet_seq = jnp.swapaxes(kpe_seq, 1, 2)
        kpe4 = jnp.tile(kpe_seq, (1, 1, 4))

        qn = jnp.einsum('btq,fq->btf', c_q, wqn, preferred_element_type=F32).astype(BF16)
        qp = jnp.einsum('btq,fq->btf', c_q, wqp, preferred_element_type=F32).astype(BF16)
        grad_o = jnp.einsum('btd,fd->btf', dy_own, wo_all, preferred_element_type=F32).astype(BF16)

        rank_arr = cp_rank.astype(jnp.int32).reshape(1)
        prev = None
        o_all = [None] * nb
        o_first = attention_fwd(0, rank_arr, qn, qp, ckv_seq, ckvt_seq, kpe4, wuk, wuv, cos128, sin128, scale)
        o_all[0] = lax.all_gather(o_first, 'tp', axis=0, tiled=True)
        for j in (*range(1, nb), 0):
            res = attention(j, rank_arr, qn, qp, grad_o, ckv_seq, ckvt_seq, kpe4, kpet_seq, wuk, wuv, cos128, sin128, prev, scale)
            prev = res[1:]
            if j:
                o_all[j] = lax.all_gather(res[0], 'tp', axis=0, tiled=True)
        dqn, dqp, dc_seq, dkp_seq, dwk, dwv = prev

        dkp_seq = dkp_seq[..., :32] + dkp_seq[..., 32:64] + dkp_seq[..., 64:96] + dkp_seq[..., 96:]
        lat = jnp.concatenate([dc_seq, dkp_seq], axis=-1)
        b0, b1, b2, b3 = (lat[:, i * half_len:(i + 1) * half_len] for i in range(4))
        outer = jnp.concatenate([b0, b3], axis=1)
        inner = jnp.concatenate([b1, b2], axis=1)
        mine = jnp.where(cp_rank == 0, outer, inner)
        theirs = jnp.where(cp_rank == 0, inner, outer)
        lat = mine + lax.ppermute(theirs, 'cp', swap_pairs)
        grad_cq = jnp.einsum('btf,fq->btq', dqn, wqn, preferred_element_type=F32) + jnp.einsum('btf,fq->btq', dqp, wqp, preferred_element_type=F32)

        norm_q_pull = jax.vjp(norm_f32, cq_f32, gq_f32)[1]
        grad_cq_raw, grad_g_q = norm_q_pull(grad_cq)
        norm_kv_pull = jax.vjp(norm_f32, ckv_f32, gkv_f32)[1]
        grad_ckv_raw, grad_g_kv = norm_kv_pull(lat[..., :kv_lora])
        grad_raw = jnp.concatenate([grad_cq_raw, grad_ckv_raw, unrope(lat[..., kv_lora:], cos_tab, sin_tab)], axis=-1).astype(BF16)
        grad_raw = lax.all_gather(grad_raw, 'tp', axis=0, tiled=True)
        part = jnp.concatenate([grad_g_q, grad_g_kv])
        part = part + lax.ppermute(part, 'cp', swap_pairs)
        parts = jnp.stack([part] + [lax.ppermute(part, 'tp', [(s, (s + k) % tp_size) for s in range(tp_size)]) for k in range(1, tp_size)])
        grad_g = sum(lax.dynamic_index_in_dim(parts, (tp_rank - s) % tp_size, 0, keepdims=False) for s in range(tp_size))

        q_half = q_lora // 2
        cq_mine = lax.dynamic_slice_in_dim(c_q, cp_rank * q_half, q_half, 2)
        cq_theirs = lax.dynamic_slice_in_dim(c_q, (1 - cp_rank) * q_half, q_half, 2)

        def dw_of(dq, cq):
            return jnp.einsum('btf,btq->fq', dq, cq, preferred_element_type=F32)

        dwqn = dw_of(dqn, cq_mine) + lax.ppermute(dw_of(dqn, cq_theirs), 'cp', swap_pairs)
        dwqp = dw_of(dqp, cq_mine) + lax.ppermute(dw_of(dqp, cq_theirs), 'cp', swap_pairs)
        c_half = kv_lora // 2
        dw_kv = jnp.stack([dwk, dwv])
        kv_mine = lax.dynamic_slice_in_dim(dw_kv, cp_rank * c_half, c_half, 1)
        kv_theirs = lax.dynamic_slice_in_dim(dw_kv, (1 - cp_rank) * c_half, c_half, 1)
        dw_kv = kv_mine + lax.ppermute(kv_theirs, 'cp', swap_pairs)
        dwqn = lax.psum_scatter(dwqn, 'tp', scatter_dimension=0, tiled=True)
        dwqp = lax.psum_scatter(dwqp, 'tp', scatter_dimension=0, tiled=True)
        dw_kv = lax.psum_scatter(dw_kv, 'tp', scatter_dimension=2, tiled=True)
        dwq = jnp.concatenate([dwqn.reshape(heads_dev, nope, q_half), dwqp.reshape(heads_dev, rope_dim, q_half)], axis=1)

        def join(part, axis):
            other = lax.ppermute(part, 'cp', swap_pairs)
            return jnp.concatenate([jnp.where(cp_rank == 0, part, other), jnp.where(cp_rank == 0, other, part)], axis=axis)

        grad_w_uq = jnp.transpose(join(dwq, 2), (2, 0, 1))
        dw_kv = join(dw_kv, 1)
        grad_w_uk = dw_kv[0].reshape(kv_lora, heads_dev, nope)
        grad_w_uv = dw_kv[1].reshape(kv_lora, heads_dev, v_dim)

        y = None
        for j in range(nb):
            y = out_proj(j, nb, o_all[j], wo_all, y)
        attn_out = y.reshape(n_batch, seq_local, dim)
        cols = heads_dev * v_dim
        o_mine = jnp.stack([lax.dynamic_slice_in_dim(o, tp_rank * cols, cols, 2) for o in o_all], axis=1).reshape(n_batch, seq_local, cols)
        dwo = jnp.einsum('btf,btd->fd', o_mine, grad_out, preferred_element_type=F32)
        grad_w_o = (dwo + lax.ppermute(dwo, 'cp', swap_pairs)).reshape(heads_dev, v_dim, dim)

        dw_cat = jnp.einsum('btd,btq->dq', hidden, grad_raw, preferred_element_type=F32)
        dw_other = lax.ppermute(dw_cat, 'cp', swap_pairs)
        grad_w_dq = dw_cat[:, :q_lora] + dw_other[:, :q_lora]
        grad_w_dkv = dw_cat[:, q_lora:] + dw_other[:, q_lora:]
        grad_hidden = jnp.einsum('btq,dq->btd', grad_raw, w_cat, preferred_element_type=F32).astype(BF16)
        return (attn_out, grad_hidden, grad_w_dq, grad_g[:q_lora], grad_w_dkv, grad_g[q_lora:], grad_w_uq, grad_w_uk, grad_w_uv, grad_w_o)

    seq_spec = P(None, 'cp', None)
    full_spec = P()
    head_spec = P(None, 'tp', None)
    out_head_spec = P('tp', None, None)
    all_specs = (seq_spec, seq_spec, full_spec, full_spec, full_spec, full_spec, head_spec, head_spec, head_spec, out_head_spec)
    return jax.shard_map(per_device, mesh=mesh, in_specs=all_specs, out_specs=all_specs, check_vma=False)
```

```python
import functools

import jax
import jax.numpy as jnp
from jax import lax
from jax.experimental import pallas as pl
from jax.experimental.pallas import tpu as pltpu
from jax.sharding import PartitionSpec as P


EPS = 1e-6
THETA = 10000.0
NEG_BIG = -1e30
LOG2E = 1.4426950408889634
F32 = jnp.float32
BF16 = jnp.bfloat16
LANES = 128
GROUP = 4
VMEM_LIMIT = 56 * 1024 * 1024

NN = (((1,), (0,)), ((), ()))
NT = (((1,), (1,)), ((), ()))


def mm(a, b, dims=NN):
    return lax.dot_general(a, b, dims, preferred_element_type=F32)


def rope_tables(positions, rope_dim):
    inv_freq = 1.0 / (THETA ** (jnp.arange(rope_dim // 2, dtype=F32) * 2.0 / rope_dim))
    angles = positions.astype(F32)[:, None] * inv_freq[None, :]
    return jnp.cos(angles), jnp.sin(angles)


def apply_rope(values, cos_tab, sin_tab):
    half_dim = values.shape[-1] // 2
    lead_half = values[..., :half_dim]
    tail_half = values[..., half_dim:]
    return jnp.concatenate([lead_half * cos_tab - tail_half * sin_tab, tail_half * cos_tab + lead_half * sin_tab], axis=-1)


def unrope(grad_vals, cos_tab, sin_tab):
    half_dim = grad_vals.shape[-1] // 2
    lead_half = grad_vals[..., :half_dim]
    tail_half = grad_vals[..., half_dim:]
    return jnp.concatenate([lead_half * cos_tab + tail_half * sin_tab, tail_half * cos_tab - lead_half * sin_tab], axis=-1)


def norm_f32(raw_vals, gain_vec):
    inv_rms = lax.rsqrt(jnp.mean(raw_vals * raw_vals, axis=-1, keepdims=True) + EPS)
    return raw_vals * inv_rms * gain_vec


def attn_kernel(grad, first, scale, *refs):
    it = iter(refs)

    def take(n):
        return [next(it) for _ in range(n)]

    rank_ref, qn_ref, qp_ref, ckv_ref, ckvt_ref, kpe_ref, wuk_ref, wuv_ref, cos_ref, sin_ref = take(10)
    if grad:
        do_ref, kpet_ref = take(2)
        if not first:
            dwk_in, dwv_in = take(6)[:2]
    o_ref = next(it)
    if grad:
        dqn_ref, dqp_ref, dc_ref, dkp_ref, dwk_ref, dwv_ref = take(6)
    k_s, vt_s, e_s, p_s, qm_s = take(5)
    if grad:
        kt_s, v_s, g_s, ds_s, dom_s, dk_s, dv_s = take(7)

    qrows = qn_ref.shape[1]
    blk = qrows // 2
    sub = blk // 2
    half = LANES // 2
    quarter = LANES // 4
    lane = lax.broadcasted_iota(jnp.int32, (1, LANES), 1)
    lane2 = lax.broadcasted_iota(jnp.int32, (1, 2 * LANES), 1)
    coef = scale * LOG2E

    ckv = ckv_ref[0]
    ckvt = ckvt_ref[0]
    wuk = wuk_ref[...]
    wuv = wuv_ref[...]
    k_s[...] = mm(ckv, wuk, NT).astype(BF16)
    vt_s[...] = mm(wuv, ckvt).astype(BF16)
    if grad:
        kt_s[...] = mm(wuk, ckvt).astype(BF16)
        v_s[...] = mm(ckv, wuv, NT).astype(BF16)

    def swap(u):
        shift = quarter // 2
        return jnp.where(lane % quarter < shift, pltpu.roll(u, LANES - shift, 1), pltpu.roll(u, shift, 1))

    qpu = qp_ref[0].astype(F32)
    cos = cos_ref[...]
    sin = sin_ref[...]
    qpr = (qpu * cos + swap(qpu) * sin).astype(BF16)
    zero = jnp.zeros((), BF16)

    def pair_lanes(h):
        return slice(h // 2 * LANES, h // 2 * LANES + LANES)

    for h in range(GROUP):
        qm_s[h, :, :LANES] = jnp.where(lane // half == h % 2, qn_ref[0, :, pair_lanes(h)], zero)
        qm_s[h, :, LANES:] = jnp.where(lane // quarter == h, qpr, zero)
        if grad:
            dom_s[h] = jnp.where(lane2 // half == h, do_ref[0], zero)

    def fold(x, op):
        return op(x.reshape(x.shape[0] // 8, 8, x.shape[1]), axis=0)

    def run(lo, hi):
        units = [(qrows - blk, hi * blk, h) for h in range(GROUP)] + [(0, lo * blk, h) for h in range(GROUP)]
        o_t = {}
        dq_t = {}

        def scores(i):
            row0, nk, h = units[i]
            kop = jnp.concatenate([k_s[:nk, pair_lanes(h)], kpe_ref[0, :nk, :]], axis=1)
            e_s[i % 2, :nk, :] = mm(kop, qm_s[h, row0:row0 + blk, :], NT)

        def dprobs(i):
            row0, nk, h = units[i]
            g_s[i % 2, :nk, :] = mm(v_s[:nk, :], dom_s[h, row0:row0 + blk, :], NT)

        def vector_passes(i):
            _, nk, h = units[i]
            slot = i % 2
            st = {}
            cols = slice(h * blk, h * blk + blk)

            def put(key, val, op):
                st[key] = op(st[key], val) if key in st else val

            def top(c):
                x = e_s[slot, c:c + sub, :]
                if c >= nk - blk:
                    key = lax.broadcasted_iota(jnp.int32, (sub, blk), 0) + (c - nk + blk)
                    x = jnp.where(key <= lax.broadcasted_iota(jnp.int32, (sub, blk), 1), x, NEG_BIG)
                    e_s[slot, c:c + sub, :] = x
                put('m', fold(x, jnp.max), jnp.maximum)

            def expo(c):
                if c == 0:
                    st['max'] = jnp.max(st['m'], axis=0, keepdims=True)
                e = jnp.exp2((e_s[slot, c:c + sub, :] - st['max']) * coef)
                e_s[slot, c:c + sub, :] = e
                put('l', fold(e, jnp.sum), jnp.add)
                if grad:
                    put('d', fold(e * g_s[slot, c:c + sub, :], jnp.sum), jnp.add)

            def probs(c):
                if c == 0:
                    st['inv'] = 1.0 / jnp.sum(st['l'], axis=0, keepdims=True)
                    if grad:
                        st['dot'] = jnp.sum(st['d'], axis=0, keepdims=True) * st['inv']
                p = e_s[slot, c:c + sub, :] * st['inv']
                p_s[c:c + sub, cols] = p.astype(BF16)
                if grad:
                    ds_s[c:c + sub, cols] = (p * (g_s[slot, c:c + sub, :] - st['dot'])).astype(BF16)

            return [functools.partial(f, c) for f in (top, expo, probs) for c in range(0, nk, sub)]

        def out(i):
            row0, nk, h = units[i]
            o_t[h] = mm(vt_s[h * half:h * half + half, :nk], p_s[:nk, h * blk:h * blk + blk])
            if h % 2:
                o_ref[0, row0:row0 + blk, pair_lanes(h)] = jnp.concatenate([o_t[h - 1], o_t[h]], axis=0).T.astype(BF16)

        def dquery(i):
            row0, nk, h = units[i]
            kop_t = jnp.concatenate([kt_s[h * half:h * half + half, :nk], kpet_ref[0, :, :nk]], axis=0)
            dq_t[h] = mm(kop_t, ds_s[:nk, h * blk:h * blk + blk])
            rows = slice(row0, row0 + blk)
            if h % 2:
                dqn_ref[0, rows, pair_lanes(h)] = (jnp.concatenate([dq_t[h - 1][:half], dq_t[h][:half]], axis=0).T * scale).astype(BF16)
            if h == GROUP - 1:
                dqp = jnp.concatenate([dq_t[g][half:] for g in range(GROUP)], axis=0).T * scale
                dqp_ref[0, rows, :] = (dqp * cos[rows] - swap(dqp) * sin[rows]).astype(BF16)

        def dkeys(i, dst, lhs, rhs):
            row0, nk, h = units[i]
            cols = slice((h - 1) * blk, (h + 1) * blk)
            val = mm(lhs[:nk, cols], jnp.concatenate([rhs[h - 1, row0:row0 + blk, :], rhs[h, row0:row0 + blk, :]], axis=0))
            if row0:
                dst[h // 2, :nk, :] = val
                if nk < dst.shape[1]:
                    dst[h // 2, nk:, :] = jnp.zeros((dst.shape[1] - nk, dst.shape[2]), F32)
            else:
                dst[h // 2, :nk, :] += val

        def before(i):
            return [functools.partial(scores, i)] + ([functools.partial(dprobs, i)] if grad else [])

        def after(i):
            work = [functools.partial(out, i)]
            if grad:
                work.append(functools.partial(dquery, i))
                if units[i][-1] % 2:
                    work.append(functools.partial(dkeys, i, dv_s, p_s, dom_s))
                    work.append(functools.partial(dkeys, i, dk_s, ds_s, qm_s))
            return work

        for f in before(0):
            f()
        for i in range(len(units)):
            vec = vector_passes(i)
            mat = (before(i + 1) if i + 1 < len(units) else []) + (after(i - 1) if i else [])
            for c, f in enumerate(vec):
                for g in mat[c * len(mat) // len(vec):(c + 1) * len(mat) // len(vec)]:
                    g()
                f()
        for f in after(len(units) - 1):
            f()

    rank = rank_ref[0]

    @pl.when(rank == 0)
    def _():
        run(1, 4)

    @pl.when(rank == 1)
    def _():
        run(2, 3)

    if grad:
        dkb = (jnp.concatenate([dk_s[0, :, :LANES], dk_s[1, :, :LANES]], axis=1) * scale).astype(BF16)
        dvb = (dv_s[0] + dv_s[1]).astype(BF16)
        dkp = (dk_s[0, :, LANES:] + dk_s[1, :, LANES:]) * scale
        dc = mm(dkb, wuk) + mm(dvb, wuv)
        dwk = mm(ckvt, dkb)
        dwv = mm(ckvt, dvb)
        dwk_ref[...] = dwk if first else dwk_in[...] + dwk
        dwv_ref[...] = dwv if first else dwv_in[...] + dwv
        step = pl.program_id(0)

        @pl.when(step == 0)
        def _():
            dc_ref[0] = dc
            dkp_ref[0] = dkp

        @pl.when(step > 0)
        def _():
            dc_ref[0] += dc
            dkp_ref[0] += dkp


def attention(j, grad_args, prev, scale, rank_arr, qn, qp, ckv, ckvt, kpe4, wuk, wuv, cos, sin):
    nb, qrows, width = qn.shape
    nkeys, latent = ckv.shape[1:]
    step = GROUP * LANES // 2
    groups = width // step
    blk = qrows // 2
    grad = grad_args is not None
    first = prev is None

    def row(cols, at=j):
        return pl.BlockSpec((1, qrows, cols), lambda i: (at, 0, i))

    def whole(*shape):
        return pl.BlockSpec((1, *shape), lambda i: (j, 0, 0))

    weight = pl.BlockSpec((step, latent), lambda i: (i, 0))
    table = pl.BlockSpec((qrows, LANES), lambda i: (0, 0))
    dweight = pl.BlockSpec((latent, step), lambda i: (0, i))
    in_specs = [pl.BlockSpec(memory_space=pltpu.SMEM), row(step), row(LANES), whole(nkeys, latent), whole(latent, nkeys), whole(nkeys, LANES), weight, weight, table, table]
    args = [rank_arr, qn, qp, ckv, ckvt, kpe4, wuk, wuv, cos, sin]
    out_specs = [row(step, 0)]
    out_shape = [jax.ShapeDtypeStruct((1, qrows, width), BF16)]
    scratch = [
        pltpu.VMEM((nkeys, step), BF16), pltpu.VMEM((step, nkeys), BF16), pltpu.VMEM((2, nkeys, blk), F32),
        pltpu.VMEM((nkeys, GROUP * blk), BF16), pltpu.VMEM((GROUP, qrows, step), BF16),
    ]
    aliases = {}
    if grad:
        in_specs += [row(step), whole(LANES // 4, nkeys)]
        args += grad_args
        if not first:
            dqn, dqp, dc, dkp, dwk, dwv = prev
            base = len(args)
            in_specs += [dweight] * 2 + [pl.BlockSpec(memory_space=pl.ANY)] * 4
            args += [dwk, dwv, dqn, dqp, dc, dkp]
            aliases = {base + i: o for i, o in enumerate((5, 6, 1, 2, 3, 4))}
        out_specs += [row(step), row(LANES), whole(nkeys, latent), whole(nkeys, LANES), dweight, dweight]
        out_shape += [
            jax.ShapeDtypeStruct((nb, qrows, width), BF16), jax.ShapeDtypeStruct((nb, qrows, width // 2), BF16),
            jax.ShapeDtypeStruct((nb, nkeys, latent), F32), jax.ShapeDtypeStruct((nb, nkeys, LANES), F32),
            jax.ShapeDtypeStruct((latent, width), F32), jax.ShapeDtypeStruct((latent, width), F32),
        ]
        scratch += [
            pltpu.VMEM((step, nkeys), BF16), pltpu.VMEM((nkeys, step), BF16), pltpu.VMEM((2, nkeys, blk), F32),
            pltpu.VMEM((nkeys, GROUP * blk), BF16), pltpu.VMEM((GROUP, qrows, step), BF16),
            pltpu.VMEM((2, nkeys, step), F32), pltpu.VMEM((2, nkeys, step), F32),
        ]
    pairs = 5 * GROUP * groups * blk * blk
    return pl.pallas_call(
        functools.partial(attn_kernel, grad, first, scale),
        grid=(groups,),
        in_specs=in_specs,
        out_specs=out_specs,
        out_shape=out_shape,
        scratch_shapes=scratch,
        input_output_aliases=aliases,
        name="attn_fwd_bwd" if grad else "attn_fwd",
        compiler_params=pltpu.CompilerParams(dimension_semantics=("arbitrary",), vmem_limit_bytes=VMEM_LIMIT),
        cost_estimate=pl.CostEstimate(flops=pairs * step * (12 if grad else 4), bytes_accessed=20 * nb * qrows * width, transcendentals=pairs),
    )(*args)


def out_kernel(o_ref, w_ref, *rest):
    y_ref = rest[-1]
    w = w_ref[...]
    for t in range(o_ref.shape[0]):
        y_ref[t, 0] = mm(o_ref[t], w).astype(BF16)


def out_proj(j, nb, o_all, w_o, prev):
    tp, rows, width = o_all.shape
    dim = w_o.shape[1]
    in_specs = [pl.BlockSpec((tp, rows, width), lambda i: (0, 0, 0)), pl.BlockSpec((width, 256), lambda i: (0, i))]
    args = [o_all, w_o]
    aliases = {}
    if prev is not None:
        in_specs.append(pl.BlockSpec(memory_space=pl.ANY))
        args.append(prev)
        aliases = {2: 0}
    return pl.pallas_call(
        out_kernel,
        grid=(dim // 256,),
        in_specs=in_specs,
        out_specs=pl.BlockSpec((tp, 1, rows, 256), lambda i: (0, j, 0, i)),
        out_shape=jax.ShapeDtypeStruct((tp, nb, rows, dim), BF16),
        input_output_aliases=aliases,
        name="out_proj",
        compiler_params=pltpu.CompilerParams(dimension_semantics=("arbitrary",), vmem_limit_bytes=VMEM_LIMIT),
        cost_estimate=pl.CostEstimate(flops=2 * tp * rows * width * dim, bytes_accessed=2 * (2 * tp * rows * width + width * dim), transcendentals=0),
    )(*args)


def dwo_kernel(tp, col_ref, *refs):
    *o_refs, dy_ref, out_ref, ot_s = refs
    step = pl.program_id(0)
    per = o_refs[0].shape[0]
    rows = o_refs[0].shape[1]
    for j, o_ref in enumerate(o_refs):
        @pl.when(step // (tp // per) == j)
        def _():
            for t in range(per):
                ot_s[:, t * rows:(t + 1) * rows] = o_ref[t].astype(F32).T.astype(BF16)

    tile = 4 * LANES
    for n in range(0, out_ref.shape[1], tile):
        cols = slice(n, n + tile)
        val = mm(ot_s[...], jnp.concatenate([dy_ref[t, 0, :, cols] for t in range(per)], axis=0))

        @pl.when(step == 0)
        def _():
            out_ref[:, cols] = val

        @pl.when(step > 0)
        def _():
            out_ref[:, cols] += val


def grad_wo(o_all, dy, cols, col_arr):
    tp, rows, _ = o_all[0].shape
    nb = len(o_all)
    dim = dy.shape[-1]
    per = 2
    turns = tp // per

    def o_spec(j):
        return pl.BlockSpec((per, rows, cols), lambda i, col: (jnp.clip(i - j * turns, 0, turns - 1), 0, col[0]))

    return pl.pallas_call(
        functools.partial(dwo_kernel, tp),
        grid_spec=pltpu.PrefetchScalarGridSpec(
            num_scalar_prefetch=1,
            grid=(nb * turns,),
            in_specs=[o_spec(j) for j in range(nb)] + [pl.BlockSpec((per, 1, rows, dim), lambda i, col: (i % turns, i // turns, 0, 0))],
            out_specs=pl.BlockSpec((cols, dim), lambda i, col: (0, 0)),
            scratch_shapes=[pltpu.VMEM((cols, per * rows), BF16)],
        ),
        out_shape=jax.ShapeDtypeStruct((cols, dim), F32),
        name="grad_wo",
        compiler_params=pltpu.CompilerParams(dimension_semantics=("arbitrary",), vmem_limit_bytes=VMEM_LIMIT),
        cost_estimate=pl.CostEstimate(flops=2 * nb * tp * rows * cols * dim, bytes_accessed=2 * nb * tp * rows * (cols + dim), transcendentals=0),
    )(col_arr, *o_all, dy.reshape(tp, nb, rows, dim))


def join_kernel(a_ref, b_ref, q_ref, kv_ref):
    split = q_ref.shape[1]
    q_ref[...] = (a_ref[:split, :] + b_ref[:split, :]).T
    kv_ref[...] = (a_ref[split:, :] + b_ref[split:, :]).T


def join_cp(a, b, split):
    wide, dim = a.shape
    tile = 2 * LANES
    part = pl.BlockSpec((wide, tile), lambda i: (0, i))
    return pl.pallas_call(
        join_kernel,
        grid=(dim // tile,),
        in_specs=[part, part],
        out_specs=[pl.BlockSpec((tile, split), lambda i: (i, 0)), pl.BlockSpec((tile, wide - split), lambda i: (i, 0))],
        out_shape=[jax.ShapeDtypeStruct((dim, split), F32), jax.ShapeDtypeStruct((dim, wide - split), F32)],
        name="join_cp",
        compiler_params=pltpu.CompilerParams(dimension_semantics=("arbitrary",), vmem_limit_bytes=VMEM_LIMIT),
        cost_estimate=pl.CostEstimate(flops=wide * dim, bytes_accessed=12 * wide * dim, transcendentals=0),
    )(a, b)


def solution(mesh):
    cp_size = mesh.shape['cp']
    tp_size = mesh.shape['tp']
    swap_pairs = [(0, 1), (1, 0)]

    def per_device(hidden, grad_out, w_dq, g_q, w_dkv, g_kv, w_uq, w_uk, w_uv, w_o):
        cp_rank = lax.axis_index('cp')
        tp_rank = lax.axis_index('tp')
        n_batch, seq_local, dim = hidden.shape
        nb = n_batch // tp_size
        q_lora = w_dq.shape[1]
        kv_lora = g_kv.shape[0]
        nope = w_uk.shape[2]
        qk_dim = w_uq.shape[2]
        rope_dim = qk_dim - nope
        heads_dev = w_uq.shape[1]
        heads = heads_dev * tp_size
        v_dim = w_uv.shape[2]
        scale = qk_dim ** -0.5
        half_len = seq_local // 2
        half_heads = heads_dev // 2

        def swapped(val):
            return lax.ppermute(val, 'cp', swap_pairs)

        def gather_weight(w):
            half = lax.dynamic_slice_in_dim(w, cp_rank * half_heads, half_heads, 0)
            return lax.all_gather(half, ('tp', 'cp'), axis=0, tiled=True)

        slabs = q_lora // kv_lora
        wq_rows = jnp.transpose(w_uq.reshape(slabs, kv_lora, heads_dev, qk_dim), (2, 0, 3, 1)).reshape(heads_dev, slabs * qk_dim, kv_lora)
        w_up = gather_weight(jnp.concatenate([wq_rows, jnp.transpose(w_uk, (1, 2, 0)), jnp.transpose(w_uv, (1, 2, 0))], axis=1))
        wo_all = gather_weight(w_o).reshape(heads * v_dim, dim)

        def q_rows(lo, hi):
            parts = [w_up[:, s * qk_dim + lo:s * qk_dim + hi] for s in range(slabs)]
            return jnp.concatenate(parts, axis=2).reshape(heads * (hi - lo), q_lora)

        wqn = q_rows(0, nope)
        wqp = q_rows(nope, qk_dim)
        wuk = w_up[:, slabs * qk_dim:slabs * qk_dim + nope].reshape(heads * nope, kv_lora)
        wuv = w_up[:, slabs * qk_dim + nope:].reshape(heads * v_dim, kv_lora)

        local_idx = jnp.arange(seq_local, dtype=jnp.int32)
        block_id = jnp.where(local_idx < half_len, cp_rank, 2 * cp_size - 1 - cp_rank)
        positions = block_id * half_len + local_idx % half_len
        cos_tab, sin_tab = rope_tables(positions, rope_dim)
        cos128 = jnp.tile(cos_tab, (1, 8))
        sin128 = jnp.tile(jnp.concatenate([-sin_tab, sin_tab], axis=1), (1, 4))

        w_cat = jnp.concatenate([w_dq, w_dkv], axis=1)
        x_own = lax.dynamic_slice_in_dim(hidden, tp_rank * nb, nb, 0)
        dy_own = lax.dynamic_slice_in_dim(grad_out, tp_rank * nb, nb, 0)

        raw = jnp.einsum('btd,dq->btq', x_own, w_cat, preferred_element_type=F32).astype(BF16)
        cq_f32 = raw[..., :q_lora].astype(F32)
        ckv_f32 = raw[..., q_lora:q_lora + kv_lora].astype(F32)
        gq_f32 = g_q.astype(F32)
        gkv_f32 = g_kv.astype(F32)
        c_q = norm_f32(cq_f32, gq_f32).astype(BF16)
        c_kv = norm_f32(ckv_f32, gkv_f32).astype(BF16)
        k_pe = apply_rope(raw[..., q_lora + kv_lora:].astype(F32), cos_tab, sin_tab).astype(BF16)

        def by_position(own, other):
            lo = jnp.where(cp_rank == 0, own[:, :half_len], other[:, :half_len])
            lo2 = jnp.where(cp_rank == 0, other[:, :half_len], own[:, :half_len])
            hi = jnp.where(cp_rank == 0, other[:, half_len:], own[:, half_len:])
            hi2 = jnp.where(cp_rank == 0, own[:, half_len:], other[:, half_len:])
            return jnp.concatenate([lo, lo2, hi, hi2], axis=1)

        other_kv, other_pe = lax.ppermute((c_kv, k_pe), 'cp', swap_pairs)
        ckv_seq = by_position(c_kv, other_kv)
        kpe_seq = by_position(k_pe, other_pe)
        ckvt_seq = jnp.swapaxes(ckv_seq, 1, 2)
        kpet_seq = jnp.swapaxes(kpe_seq, 1, 2)
        kpe4 = jnp.tile(kpe_seq, (1, 1, 4))

        qn = jnp.einsum('btq,fq->btf', c_q, wqn, preferred_element_type=F32).astype(BF16)
        qp = jnp.einsum('btq,fq->btf', c_q, wqp, preferred_element_type=F32).astype(BF16)
        grad_o = jnp.einsum('btd,fd->btf', dy_own, wo_all, preferred_element_type=F32).astype(BF16)

        rank_arr = cp_rank.astype(jnp.int32).reshape(1)
        attn_args = (rank_arr, qn, qp, ckv_seq, ckvt_seq, kpe4, wuk, wuv, cos128, sin128)
        prev = None
        o_all = [None] * nb
        o_first = attention(0, None, None, scale, *attn_args)[0]
        o_all[0] = lax.all_gather(o_first, 'tp', axis=0, tiled=True)
        for j in (*range(1, nb), 0):
            res = attention(j, [grad_o, kpet_seq], prev, scale, *attn_args)
            prev = res[1:]
            if j:
                o_all[j] = lax.all_gather(res[0], 'tp', axis=0, tiled=True)
        dqn, dqp, dc_seq, dkp_seq, dwk, dwv = prev

        dkp_seq = dkp_seq[..., :32] + dkp_seq[..., 32:64] + dkp_seq[..., 64:96] + dkp_seq[..., 96:]
        lat = jnp.concatenate([dc_seq, dkp_seq], axis=-1)
        b0, b1, b2, b3 = (lat[:, i * half_len:(i + 1) * half_len] for i in range(4))
        outer = jnp.concatenate([b0, b3], axis=1)
        inner = jnp.concatenate([b1, b2], axis=1)
        mine = jnp.where(cp_rank == 0, outer, inner)
        theirs = jnp.where(cp_rank == 0, inner, outer)
        lat = mine + lax.ppermute(theirs, 'cp', swap_pairs)
        grad_cq = jnp.einsum('btf,fq->btq', dqn, wqn, preferred_element_type=F32) + jnp.einsum('btf,fq->btq', dqp, wqp, preferred_element_type=F32)

        norm_q_pull = jax.vjp(norm_f32, cq_f32, gq_f32)[1]
        grad_cq_raw, grad_g_q = norm_q_pull(grad_cq)
        norm_kv_pull = jax.vjp(norm_f32, ckv_f32, gkv_f32)[1]
        grad_ckv_raw, grad_g_kv = norm_kv_pull(lat[..., :kv_lora])
        grad_raw = jnp.concatenate([grad_cq_raw, grad_ckv_raw, unrope(lat[..., kv_lora:], cos_tab, sin_tab)], axis=-1).astype(BF16)
        grad_raw = lax.all_gather(grad_raw, 'tp', axis=0, tiled=True)
        part = jnp.concatenate([grad_g_q, grad_g_kv])
        part = part + swapped(part)
        parts = jnp.stack([part] + [lax.ppermute(part, 'tp', [(s, (s + k) % tp_size) for s in range(tp_size)]) for k in range(1, tp_size)])
        grad_g = sum(lax.dynamic_index_in_dim(parts, (tp_rank - s) % tp_size, 0, keepdims=False) for s in range(tp_size))

        q_half = q_lora // 2
        cq_mine = lax.dynamic_slice_in_dim(c_q, cp_rank * q_half, q_half, 2)
        cq_theirs = lax.dynamic_slice_in_dim(c_q, (1 - cp_rank) * q_half, q_half, 2)

        def dw_of(dq, cq):
            return jnp.einsum('btf,btq->fq', dq, cq, preferred_element_type=F32)

        dwqn = dw_of(dqn, cq_mine) + swapped(dw_of(dqn, cq_theirs))
        dwqp = dw_of(dqp, cq_mine) + swapped(dw_of(dqp, cq_theirs))
        c_half = kv_lora // 2
        dw_kv = jnp.stack([dwk, dwv])
        kv_mine = lax.dynamic_slice_in_dim(dw_kv, cp_rank * c_half, c_half, 1)
        kv_theirs = lax.dynamic_slice_in_dim(dw_kv, (1 - cp_rank) * c_half, c_half, 1)
        dw_kv = kv_mine + swapped(kv_theirs)
        dwqn = lax.psum_scatter(dwqn, 'tp', scatter_dimension=0, tiled=True)
        dwqp = lax.psum_scatter(dwqp, 'tp', scatter_dimension=0, tiled=True)
        dw_kv = lax.psum_scatter(dw_kv, 'tp', scatter_dimension=2, tiled=True)
        dwq = jnp.concatenate([dwqn.reshape(heads_dev, nope, q_half), dwqp.reshape(heads_dev, rope_dim, q_half)], axis=1)

        def join(part, axis):
            other = lax.ppermute(part, 'cp', swap_pairs)
            return jnp.concatenate([jnp.where(cp_rank == 0, part, other), jnp.where(cp_rank == 0, other, part)], axis=axis)

        grad_w_uq = jnp.transpose(join(dwq, 2), (2, 0, 1))
        dw_kv = join(dw_kv, 1)
        grad_w_uk = dw_kv[0].reshape(kv_lora, heads_dev, nope)
        grad_w_uv = dw_kv[1].reshape(kv_lora, heads_dev, v_dim)

        y = None
        for j in range(nb):
            y = out_proj(j, nb, o_all[j], wo_all, y)
        attn_out = y.reshape(n_batch, seq_local, dim)
        cols = heads_dev * v_dim
        dwo = grad_wo(o_all, grad_out, cols, tp_rank.astype(jnp.int32).reshape(1))
        grad_w_o = (dwo + lax.ppermute(dwo, 'cp', swap_pairs)).reshape(heads_dev, v_dim, dim)

        dw_cat = jnp.einsum('btq,btd->qd', grad_raw, hidden, preferred_element_type=F32)
        grad_w_dq, grad_w_dkv = join_cp(dw_cat, lax.ppermute(dw_cat, 'cp', swap_pairs), q_lora)
        grad_hidden = jnp.einsum('btq,dq->btd', grad_raw, w_cat, preferred_element_type=F32).astype(BF16)
        return (attn_out, grad_hidden, grad_w_dq, grad_g[:q_lora], grad_w_dkv, grad_g[q_lora:], grad_w_uq, grad_w_uk, grad_w_uv, grad_w_o)

    seq_spec = P(None, 'cp', None)
    full_spec = P()
    head_spec = P(None, 'tp', None)
    out_head_spec = P('tp', None, None)
    all_specs = (seq_spec, seq_spec, full_spec, full_spec, full_spec, full_spec, head_spec, head_spec, head_spec, out_head_spec)
    return jax.shard_map(per_device, mesh=mesh, in_specs=all_specs, out_specs=all_specs, check_vma=False)
```

```python
import functools

import jax
import jax.numpy as jnp
from jax import lax
from jax.experimental import pallas as pl
from jax.experimental.pallas import tpu as pltpu
from jax.sharding import PartitionSpec as P


EPS = 1e-6
THETA = 10000.0
NEG_BIG = -1e30
LOG2E = 1.4426950408889634
F32 = jnp.float32
BF16 = jnp.bfloat16
LANES = 128
GROUP = 4
VMEM_LIMIT = 56 * 1024 * 1024

NN = (((1,), (0,)), ((), ()))
NT = (((1,), (1,)), ((), ()))


def mm(a, b, dims=NN):
    return lax.dot_general(a, b, dims, preferred_element_type=F32)


def rope_tables(positions, rope_dim):
    inv_freq = 1.0 / (THETA ** (jnp.arange(rope_dim // 2, dtype=F32) * 2.0 / rope_dim))
    angles = positions.astype(F32)[:, None] * inv_freq[None, :]
    return jnp.cos(angles), jnp.sin(angles)


def apply_rope(values, cos_tab, sin_tab):
    half_dim = values.shape[-1] // 2
    lead_half = values[..., :half_dim]
    tail_half = values[..., half_dim:]
    return jnp.concatenate([lead_half * cos_tab - tail_half * sin_tab, tail_half * cos_tab + lead_half * sin_tab], axis=-1)


def unrope(grad_vals, cos_tab, sin_tab):
    half_dim = grad_vals.shape[-1] // 2
    lead_half = grad_vals[..., :half_dim]
    tail_half = grad_vals[..., half_dim:]
    return jnp.concatenate([lead_half * cos_tab + tail_half * sin_tab, tail_half * cos_tab - lead_half * sin_tab], axis=-1)


def norm_f32(raw_vals, gain_vec):
    inv_rms = lax.rsqrt(jnp.mean(raw_vals * raw_vals, axis=-1, keepdims=True) + EPS)
    return raw_vals * inv_rms * gain_vec


def attn_kernel(grad, first, scale, *refs):
    it = iter(refs)

    def take(n):
        return [next(it) for _ in range(n)]

    rank_ref, qn_ref, qp_ref, ckv_ref, ckvt_ref, kpe_ref, wuk_ref, wuv_ref, cos_ref, sin_ref = take(10)
    if grad:
        do_ref, kpet_ref = take(2)
        if not first:
            dwk_in, dwv_in = take(6)[:2]
    o_ref = next(it)
    if grad:
        dqn_ref, dqp_ref, dc_ref, dkp_ref, dwk_ref, dwv_ref = take(6)
    k_s, vt_s, e_s, p_s, qm_s = take(5)
    if grad:
        kt_s, v_s, g_s, ds_s, dom_s, dk_s, dv_s, dqp_s = take(8)

    qrows = qn_ref.shape[1]
    blk = qrows // 2
    sub = blk // 2
    half = LANES // 2
    quarter = LANES // 4
    lane = lax.broadcasted_iota(jnp.int32, (1, LANES), 1)
    lane2 = lax.broadcasted_iota(jnp.int32, (1, 2 * LANES), 1)
    coef = scale * LOG2E

    ckv = ckv_ref[0]
    ckvt = ckvt_ref[0]
    wuk = wuk_ref[...]
    wuv = wuv_ref[...]
    k_s[...] = mm(ckv, wuk, NT).astype(BF16)
    vt_s[...] = mm(wuv, ckvt).astype(BF16)
    if grad:
        kt_s[...] = mm(wuk, ckvt).astype(BF16)
        v_s[...] = mm(ckv, wuv, NT).astype(BF16)

    def swap(u):
        shift = quarter // 2
        return jnp.where(lane % quarter < shift, pltpu.roll(u, LANES - shift, 1), pltpu.roll(u, shift, 1))

    qpu = qp_ref[0].astype(F32)
    cos = cos_ref[...]
    sin = sin_ref[...]
    qpr = (qpu * cos + swap(qpu) * sin).astype(BF16)
    zero = jnp.zeros((), BF16)

    def pair_lanes(h):
        return slice(h // 2 * LANES, h // 2 * LANES + LANES)

    for h in range(GROUP):
        qm_s[h, :, :LANES] = jnp.where(lane // half == h % 2, qn_ref[0, :, pair_lanes(h)], zero)
        qm_s[h, :, LANES:] = jnp.where(lane // quarter == h, qpr, zero)
        if grad:
            dom_s[h] = jnp.where(lane2 // half == h, do_ref[0], zero)

    def fold(x, op):
        return op(x.reshape(x.shape[0] // 8, 8, x.shape[1]), axis=0)

    def run(lo, hi):
        units = [(qrows - blk, hi * blk, h) for h in range(GROUP)] + [(0, lo * blk, h) for h in range(GROUP)]

        def scores(i):
            row0, nk, h = units[i]
            kop = jnp.concatenate([k_s[:nk, pair_lanes(h)], kpe_ref[0, :nk, :]], axis=1)
            e_s[i % 2, :nk, :] = mm(kop, qm_s[h, row0:row0 + blk, :], NT)

        def dprobs(i):
            row0, nk, h = units[i]
            g_s[i % 2, :nk, :] = mm(v_s[:nk, pair_lanes(h)], dom_s[h, row0:row0 + blk, pair_lanes(h)], NT)

        def vector_passes(i):
            _, nk, h = units[i]
            slot = i % 2
            st = {}
            cols = slice(h * blk, h * blk + blk)

            def put(key, val, op):
                st[key] = op(st[key], val) if key in st else val

            def top(c):
                x = e_s[slot, c:c + sub, :]
                if c >= nk - blk:
                    key = lax.broadcasted_iota(jnp.int32, (sub, blk), 0) + (c - nk + blk)
                    x = jnp.where(key <= lax.broadcasted_iota(jnp.int32, (sub, blk), 1), x, NEG_BIG)
                    e_s[slot, c:c + sub, :] = x
                put('m', fold(x, jnp.max), jnp.maximum)

            def expo(c):
                if c == 0:
                    st['max'] = jnp.max(st['m'], axis=0, keepdims=True)
                e = jnp.exp2((e_s[slot, c:c + sub, :] - st['max']) * coef)
                e_s[slot, c:c + sub, :] = e
                put('l', fold(e, jnp.sum), jnp.add)
                if grad:
                    put('d', fold(e * g_s[slot, c:c + sub, :], jnp.sum), jnp.add)

            def probs(c):
                if c == 0:
                    st['inv'] = 1.0 / jnp.sum(st['l'], axis=0, keepdims=True)
                    if grad:
                        st['dot'] = jnp.sum(st['d'], axis=0, keepdims=True) * st['inv']
                p = e_s[slot, c:c + sub, :] * st['inv']
                p_s[c:c + sub, cols] = p.astype(BF16)
                if grad:
                    ds_s[c:c + sub, cols] = (p * (g_s[slot, c:c + sub, :] - st['dot'])).astype(BF16)

            return [functools.partial(f, c) for f in (top, expo, probs) for c in range(0, nk, sub)]

        def out(i):
            row0, nk, h = units[i]
            parts = [mm(vt_s[g * half:g * half + half, :nk], p_s[:nk, g * blk:g * blk + blk]) for g in (h - 1, h)]
            o_ref[0, row0:row0 + blk, pair_lanes(h)] = jnp.concatenate(parts, axis=0).T.astype(BF16)

        def dquery(i):
            row0, nk, h = units[i]
            rows = slice(row0, row0 + blk)
            parts = []
            for g in (h - 1, h):
                kop_t = jnp.concatenate([kt_s[g * half:g * half + half, :nk], kpet_ref[0, :, :nk]], axis=0)
                dq = mm(kop_t, ds_s[:nk, g * blk:g * blk + blk])
                parts.append(dq[:half])
                dqp_s[g * quarter:g * quarter + quarter, :] = dq[half:]
            dqn_ref[0, rows, pair_lanes(h)] = (jnp.concatenate(parts, axis=0).T * scale).astype(BF16)
            if h == GROUP - 1:
                dqp = dqp_s[...].T * scale
                dqp_ref[0, rows, :] = (dqp * cos_ref[rows, :] - swap(dqp) * sin_ref[rows, :]).astype(BF16)

        def dkeys(i, dst, lhs, rhs):
            row0, nk, h = units[i]
            cols = slice((h - 1) * blk, (h + 1) * blk)
            val = mm(lhs[:nk, cols], jnp.concatenate([rhs[h - 1, row0:row0 + blk, :], rhs[h, row0:row0 + blk, :]], axis=0))
            if row0:
                dst[h // 2, :nk, :] = val
                if nk < dst.shape[1]:
                    dst[h // 2, nk:, :] = jnp.zeros((dst.shape[1] - nk, dst.shape[2]), F32)
            else:
                dst[h // 2, :nk, :] += val

        def before(i):
            return [functools.partial(scores, i)] + ([functools.partial(dprobs, i)] if grad else [])

        def after(i):
            return [functools.partial(out, i)] + ([functools.partial(dquery, i)] if grad else [])

        def after_keys(i):
            return [functools.partial(dkeys, i, dv_s, p_s, dom_s), functools.partial(dkeys, i, dk_s, ds_s, qm_s)] if grad else []

        def region(i):
            for u in (i, i + 1):
                vec = vector_passes(u)
                mat = before(u + 1) if u + 1 < len(units) else []
                if i:
                    mat = mat + (after(i - 1) if u == i else after_keys(i - 1))
                for c, f in enumerate(vec):
                    for g in mat[c * len(mat) // len(vec):(c + 1) * len(mat) // len(vec)]:
                        g()
                    f()

        for f in before(0):
            f()
        for i in range(0, len(units), 2):
            region(i)
        for f in after(len(units) - 1) + after_keys(len(units) - 1):
            f()

    rank = rank_ref[0]

    @pl.when(rank == 0)
    def _():
        run(1, 4)

    @pl.when(rank == 1)
    def _():
        run(2, 3)

    if grad:
        dkb = (jnp.concatenate([dk_s[0, :, :LANES], dk_s[1, :, :LANES]], axis=1) * scale).astype(BF16)
        dvb = (dv_s[0] + dv_s[1]).astype(BF16)
        dkp = (dk_s[0, :, LANES:] + dk_s[1, :, LANES:]) * scale
        dc = mm(dkb, wuk) + mm(dvb, wuv)
        dwk = mm(ckvt, dkb)
        dwv = mm(ckvt, dvb)
        dwk_ref[...] = dwk if first else dwk_in[...] + dwk
        dwv_ref[...] = dwv if first else dwv_in[...] + dwv
        step = pl.program_id(0)

        @pl.when(step == 0)
        def _():
            dc_ref[0] = dc
            dkp_ref[0] = dkp

        @pl.when(step > 0)
        def _():
            dc_ref[0] += dc
            dkp_ref[0] += dkp


def attention(j, grad_args, prev, scale, rank_arr, qn, qp, ckv, ckvt, kpe4, wuk, wuv, cos, sin):
    nb, qrows, width = qn.shape
    nkeys, latent = ckv.shape[1:]
    step = GROUP * LANES // 2
    groups = width // step
    blk = qrows // 2
    grad = grad_args is not None
    first = prev is None

    def row(cols, at=j):
        return pl.BlockSpec((1, qrows, cols), lambda i: (at, 0, i))

    def whole(*shape):
        return pl.BlockSpec((1, *shape), lambda i: (j, 0, 0))

    weight = pl.BlockSpec((step, latent), lambda i: (i, 0))
    table = pl.BlockSpec((qrows, LANES), lambda i: (0, 0))
    dweight = pl.BlockSpec((latent, step), lambda i: (0, i))
    in_specs = [pl.BlockSpec(memory_space=pltpu.SMEM), row(step), row(LANES), whole(nkeys, latent), whole(latent, nkeys), whole(nkeys, LANES), weight, weight, table, table]
    args = [rank_arr, qn, qp, ckv, ckvt, kpe4, wuk, wuv, cos, sin]
    out_specs = [row(step, 0)]
    out_shape = [jax.ShapeDtypeStruct((1, qrows, width), BF16)]
    scratch = [
        pltpu.VMEM((nkeys, step), BF16), pltpu.VMEM((step, nkeys), BF16), pltpu.VMEM((2, nkeys, blk), F32),
        pltpu.VMEM((nkeys, GROUP * blk), BF16), pltpu.VMEM((GROUP, qrows, step), BF16),
    ]
    aliases = {}
    if grad:
        in_specs += [row(step), whole(LANES // 4, nkeys)]
        args += grad_args
        if not first:
            dqn, dqp, dc, dkp, dwk, dwv = prev
            base = len(args)
            in_specs += [dweight] * 2 + [pl.BlockSpec(memory_space=pl.ANY)] * 4
            args += [dwk, dwv, dqn, dqp, dc, dkp]
            aliases = {base + i: o for i, o in enumerate((5, 6, 1, 2, 3, 4))}
        out_specs += [row(step), row(LANES), whole(nkeys, latent), whole(nkeys, LANES), dweight, dweight]
        out_shape += [
            jax.ShapeDtypeStruct((nb, qrows, width), BF16), jax.ShapeDtypeStruct((nb, qrows, width // 2), BF16),
            jax.ShapeDtypeStruct((nb, nkeys, latent), F32), jax.ShapeDtypeStruct((nb, nkeys, LANES), F32),
            jax.ShapeDtypeStruct((latent, width), F32), jax.ShapeDtypeStruct((latent, width), F32),
        ]
        scratch += [
            pltpu.VMEM((step, nkeys), BF16), pltpu.VMEM((nkeys, step), BF16), pltpu.VMEM((2, nkeys, blk), F32),
            pltpu.VMEM((nkeys, GROUP * blk), BF16), pltpu.VMEM((GROUP, qrows, step), BF16),
            pltpu.VMEM((2, nkeys, step), F32), pltpu.VMEM((2, nkeys, step), F32), pltpu.VMEM((LANES, blk), F32),
        ]
    pairs = 5 * GROUP * groups * blk * blk
    return pl.pallas_call(
        functools.partial(attn_kernel, grad, first, scale),
        grid=(groups,),
        in_specs=in_specs,
        out_specs=out_specs,
        out_shape=out_shape,
        scratch_shapes=scratch,
        input_output_aliases=aliases,
        name="attn_fwd_bwd" if grad else "attn_fwd",
        compiler_params=pltpu.CompilerParams(dimension_semantics=("arbitrary",), vmem_limit_bytes=VMEM_LIMIT),
        cost_estimate=pl.CostEstimate(flops=pairs * step * (12 if grad else 4), bytes_accessed=20 * nb * qrows * width, transcendentals=pairs),
    )(*args)


def out_kernel(o_ref, w_ref, *rest):
    y_ref = rest[-1]
    w = w_ref[...]
    for t in range(o_ref.shape[0]):
        y_ref[t, 0] = mm(o_ref[t], w).astype(BF16)


def out_proj(j, nb, o_all, w_o, prev):
    tp, rows, width = o_all.shape
    dim = w_o.shape[1]
    tile = 4 * LANES
    in_specs = [pl.BlockSpec((tp, rows, width), lambda i: (0, 0, 0)), pl.BlockSpec((width, tile), lambda i: (0, i))]
    args = [o_all, w_o]
    aliases = {}
    if prev is not None:
        in_specs.append(pl.BlockSpec(memory_space=pl.ANY))
        args.append(prev)
        aliases = {2: 0}
    return pl.pallas_call(
        out_kernel,
        grid=(dim // tile,),
        in_specs=in_specs,
        out_specs=pl.BlockSpec((tp, 1, rows, tile), lambda i: (0, j, 0, i)),
        out_shape=jax.ShapeDtypeStruct((tp, nb, rows, dim), BF16),
        input_output_aliases=aliases,
        name="out_proj",
        compiler_params=pltpu.CompilerParams(dimension_semantics=("arbitrary",), vmem_limit_bytes=VMEM_LIMIT),
        cost_estimate=pl.CostEstimate(flops=2 * tp * rows * width * dim, bytes_accessed=2 * (2 * tp * rows * width + width * dim), transcendentals=0),
    )(*args)


def dwo_kernel(tp, col_ref, *refs):
    *o_refs, dy_ref, out_ref, ot_s = refs
    step = pl.program_id(0)
    per = o_refs[0].shape[0]
    rows = o_refs[0].shape[1]
    for j, o_ref in enumerate(o_refs):
        @pl.when(step // (tp // per) == j)
        def _():
            for t in range(per):
                ot_s[:, t * rows:(t + 1) * rows] = o_ref[t].astype(F32).T.astype(BF16)

    tile = 4 * LANES
    for n in range(0, out_ref.shape[1], tile):
        cols = slice(n, n + tile)
        val = mm(ot_s[...], jnp.concatenate([dy_ref[t, 0, :, cols] for t in range(per)], axis=0))

        @pl.when(step == 0)
        def _():
            out_ref[:, cols] = val

        @pl.when(step > 0)
        def _():
            out_ref[:, cols] += val


def grad_wo(o_all, dy, cols, col_arr):
    tp, rows, _ = o_all[0].shape
    nb = len(o_all)
    dim = dy.shape[-1]
    per = tp
    turns = tp // per

    def o_spec(j):
        return pl.BlockSpec((per, rows, cols), lambda i, col: (jnp.clip(i - j * turns, 0, turns - 1), 0, col[0]))

    return pl.pallas_call(
        functools.partial(dwo_kernel, tp),
        grid_spec=pltpu.PrefetchScalarGridSpec(
            num_scalar_prefetch=1,
            grid=(nb * turns,),
            in_specs=[o_spec(j) for j in range(nb)] + [pl.BlockSpec((per, 1, rows, dim), lambda i, col: (i % turns, i // turns, 0, 0))],
            out_specs=pl.BlockSpec((cols, dim), lambda i, col: (0, 0)),
            scratch_shapes=[pltpu.VMEM((cols, per * rows), BF16)],
        ),
        out_shape=jax.ShapeDtypeStruct((cols, dim), F32),
        name="grad_wo",
        compiler_params=pltpu.CompilerParams(dimension_semantics=("arbitrary",), vmem_limit_bytes=VMEM_LIMIT * 9 // 8),
        cost_estimate=pl.CostEstimate(flops=2 * nb * tp * rows * cols * dim, bytes_accessed=2 * nb * tp * rows * (cols + dim), transcendentals=0),
    )(col_arr, *o_all, dy.reshape(tp, nb, rows, dim))


def join_kernel(a_ref, b_ref, q_ref, kv_ref):
    split = q_ref.shape[1]
    q_ref[...] = (a_ref[:split, :] + b_ref[:split, :]).T
    kv_ref[...] = a_ref[split:, :] + b_ref[split:, :]


def join_cp(a, b, split):
    wide, dim = a.shape
    tile = 2 * LANES
    part = pl.BlockSpec((wide, tile), lambda i: (0, i))
    return pl.pallas_call(
        join_kernel,
        grid=(dim // tile,),
        in_specs=[part, part],
        out_specs=[pl.BlockSpec((tile, split), lambda i: (i, 0)), pl.BlockSpec((wide - split, tile), lambda i: (0, i))],
        out_shape=[jax.ShapeDtypeStruct((dim, split), F32), jax.ShapeDtypeStruct((wide - split, dim), F32)],
        name="join_cp",
        compiler_params=pltpu.CompilerParams(dimension_semantics=("arbitrary",), vmem_limit_bytes=VMEM_LIMIT),
        cost_estimate=pl.CostEstimate(flops=wide * dim, bytes_accessed=12 * wide * dim, transcendentals=0),
    )(a, b)


def solution(mesh):
    cp_size = mesh.shape['cp']
    tp_size = mesh.shape['tp']
    swap_pairs = [(0, 1), (1, 0)]

    def per_device(hidden, grad_out, w_dq, g_q, w_dkv, g_kv, w_uq, w_uk, w_uv, w_o):
        cp_rank = lax.axis_index('cp')
        tp_rank = lax.axis_index('tp')
        n_batch, seq_local, dim = hidden.shape
        nb = n_batch // tp_size
        q_lora = w_dq.shape[1]
        kv_lora = g_kv.shape[0]
        nope = w_uk.shape[2]
        qk_dim = w_uq.shape[2]
        rope_dim = qk_dim - nope
        heads_dev = w_uq.shape[1]
        heads = heads_dev * tp_size
        v_dim = w_uv.shape[2]
        scale = qk_dim ** -0.5
        half_len = seq_local // 2
        half_heads = heads_dev // 2

        def swapped(val):
            return lax.ppermute(val, 'cp', swap_pairs)

        def own_half(w):
            return lax.dynamic_slice_in_dim(w, cp_rank * half_heads, half_heads, 0)

        def gather_weight(half):
            return lax.all_gather(half, ('tp', 'cp'), axis=0, tiled=True)

        slabs = q_lora // kv_lora
        wq_rows = own_half(jnp.transpose(w_uq, (1, 2, 0)))
        up_rows = [wq_rows[..., s * kv_lora:(s + 1) * kv_lora] for s in range(slabs)]
        up_rows += [own_half(jnp.transpose(w, (1, 2, 0))) for w in (w_uk, w_uv)]
        w_up = gather_weight(jnp.concatenate(up_rows, axis=1))
        wo_all = gather_weight(own_half(w_o)).reshape(heads * v_dim, dim)

        def q_rows(lo, hi):
            parts = [w_up[:, s * qk_dim + lo:s * qk_dim + hi] for s in range(slabs)]
            return jnp.concatenate(parts, axis=2).reshape(heads * (hi - lo), q_lora)

        wqn = q_rows(0, nope)
        wqp = q_rows(nope, qk_dim)
        wuk = w_up[:, slabs * qk_dim:slabs * qk_dim + nope].reshape(heads * nope, kv_lora)
        wuv = w_up[:, slabs * qk_dim + nope:].reshape(heads * v_dim, kv_lora)

        local_idx = jnp.arange(seq_local, dtype=jnp.int32)
        block_id = jnp.where(local_idx < half_len, cp_rank, 2 * cp_size - 1 - cp_rank)
        positions = block_id * half_len + local_idx % half_len
        cos_tab, sin_tab = rope_tables(positions, rope_dim)
        cos128 = jnp.tile(cos_tab, (1, 8))
        sin128 = jnp.tile(jnp.concatenate([-sin_tab, sin_tab], axis=1), (1, 4))

        w_cat = jnp.concatenate([w_dq, w_dkv], axis=1)
        x_own = lax.dynamic_slice_in_dim(hidden, tp_rank * nb, nb, 0)
        dy_own = lax.dynamic_slice_in_dim(grad_out, tp_rank * nb, nb, 0)

        raw = jnp.einsum('btd,dq->btq', x_own, w_cat, preferred_element_type=F32).astype(BF16)
        cq_f32 = raw[..., :q_lora].astype(F32)
        ckv_f32 = raw[..., q_lora:q_lora + kv_lora].astype(F32)
        gq_f32 = g_q.astype(F32)
        gkv_f32 = g_kv.astype(F32)
        c_q = norm_f32(cq_f32, gq_f32).astype(BF16)
        c_kv = norm_f32(ckv_f32, gkv_f32).astype(BF16)
        k_pe = apply_rope(raw[..., q_lora + kv_lora:].astype(F32), cos_tab, sin_tab).astype(BF16)

        def by_position(own, other):
            lo = jnp.where(cp_rank == 0, own[:, :half_len], other[:, :half_len])
            lo2 = jnp.where(cp_rank == 0, other[:, :half_len], own[:, :half_len])
            hi = jnp.where(cp_rank == 0, other[:, half_len:], own[:, half_len:])
            hi2 = jnp.where(cp_rank == 0, own[:, half_len:], other[:, half_len:])
            return jnp.concatenate([lo, lo2, hi, hi2], axis=1)

        other_kv, other_pe = lax.ppermute((c_kv, k_pe), 'cp', swap_pairs)
        ckv_seq = by_position(c_kv, other_kv)
        kpe_seq = by_position(k_pe, other_pe)
        ckvt_seq = jnp.swapaxes(ckv_seq, 1, 2)
        kpet_seq = jnp.swapaxes(kpe_seq, 1, 2)
        kpe4 = jnp.tile(kpe_seq, (1, 1, 4))

        qn = jnp.einsum('btq,fq->btf', c_q, wqn, preferred_element_type=F32).astype(BF16)
        qp = jnp.einsum('btq,fq->btf', c_q, wqp, preferred_element_type=F32).astype(BF16)
        grad_o = jnp.einsum('btd,fd->btf', dy_own, wo_all, preferred_element_type=F32).astype(BF16)

        rank_arr = cp_rank.astype(jnp.int32).reshape(1)
        attn_args = (rank_arr, qn, qp, ckv_seq, ckvt_seq, kpe4, wuk, wuv, cos128, sin128)
        prev = None
        o_all = [None] * nb
        o_first = attention(0, None, None, scale, *attn_args)[0]
        o_all[0] = lax.all_gather(o_first, 'tp', axis=0, tiled=True)
        for j in (*range(1, nb), 0):
            res = attention(j, [grad_o, kpet_seq], prev, scale, *attn_args)
            prev = res[1:]
            if j:
                o_all[j] = lax.all_gather(res[0], 'tp', axis=0, tiled=True)
        dqn, dqp, dc_seq, dkp_seq, dwk, dwv = prev

        dkp_seq = dkp_seq[..., :32] + dkp_seq[..., 32:64] + dkp_seq[..., 64:96] + dkp_seq[..., 96:]
        lat = jnp.concatenate([dc_seq, dkp_seq], axis=-1)
        b0, b1, b2, b3 = (lat[:, i * half_len:(i + 1) * half_len] for i in range(4))
        outer = jnp.concatenate([b0, b3], axis=1)
        inner = jnp.concatenate([b1, b2], axis=1)
        mine = jnp.where(cp_rank == 0, outer, inner)
        theirs = jnp.where(cp_rank == 0, inner, outer)
        lat = mine + lax.ppermute(theirs, 'cp', swap_pairs)
        grad_cq = jnp.einsum('btf,fq->btq', dqn, wqn, preferred_element_type=F32) + jnp.einsum('btf,fq->btq', dqp, wqp, preferred_element_type=F32)

        norm_q_pull = jax.vjp(norm_f32, cq_f32, gq_f32)[1]
        grad_cq_raw, grad_g_q = norm_q_pull(grad_cq)
        norm_kv_pull = jax.vjp(norm_f32, ckv_f32, gkv_f32)[1]
        grad_ckv_raw, grad_g_kv = norm_kv_pull(lat[..., :kv_lora])
        grad_raw = jnp.concatenate([grad_cq_raw, grad_ckv_raw, unrope(lat[..., kv_lora:], cos_tab, sin_tab)], axis=-1).astype(BF16)
        grad_raw = lax.all_gather(grad_raw, 'tp', axis=0, tiled=True)
        part = jnp.concatenate([grad_g_q, grad_g_kv])
        part = part + swapped(part)
        parts = jnp.stack([part] + [lax.ppermute(part, 'tp', [(s, (s + k) % tp_size) for s in range(tp_size)]) for k in range(1, tp_size)])
        grad_g = sum(lax.dynamic_index_in_dim(parts, (tp_rank - s) % tp_size, 0, keepdims=False) for s in range(tp_size))

        q_half = q_lora // 2
        cq_mine = lax.dynamic_slice_in_dim(c_q, cp_rank * q_half, q_half, 2)
        cq_theirs = lax.dynamic_slice_in_dim(c_q, (1 - cp_rank) * q_half, q_half, 2)

        def dw_of(dq, cq):
            return jnp.einsum('btf,btq->fq', dq, cq, preferred_element_type=F32)

        dwqn = dw_of(dqn, cq_mine) + swapped(dw_of(dqn, cq_theirs))
        dwqp = dw_of(dqp, cq_mine) + swapped(dw_of(dqp, cq_theirs))
        c_half = kv_lora // 2
        dw_kv = jnp.stack([dwk, dwv])
        kv_mine = lax.dynamic_slice_in_dim(dw_kv, cp_rank * c_half, c_half, 1)
        kv_theirs = lax.dynamic_slice_in_dim(dw_kv, (1 - cp_rank) * c_half, c_half, 1)
        dw_kv = kv_mine + swapped(kv_theirs)
        dwqn = lax.psum_scatter(dwqn, 'tp', scatter_dimension=0, tiled=True)
        dwqp = lax.psum_scatter(dwqp, 'tp', scatter_dimension=0, tiled=True)
        dw_kv = lax.psum_scatter(dw_kv, 'tp', scatter_dimension=2, tiled=True)
        dwq = jnp.concatenate([dwqn.reshape(heads_dev, nope, q_half), dwqp.reshape(heads_dev, rope_dim, q_half)], axis=1)

        def join(part, axis):
            other = lax.ppermute(part, 'cp', swap_pairs)
            return jnp.concatenate([jnp.where(cp_rank == 0, part, other), jnp.where(cp_rank == 0, other, part)], axis=axis)

        grad_w_uq = jnp.transpose(join(dwq, 2), (2, 0, 1))
        dw_kv = join(dw_kv, 1)
        grad_w_uk = dw_kv[0].reshape(kv_lora, heads_dev, nope)
        grad_w_uv = dw_kv[1].reshape(kv_lora, heads_dev, v_dim)

        y = None
        for j in range(nb):
            y = out_proj(j, nb, o_all[j], wo_all, y)
        attn_out = y.reshape(n_batch, seq_local, dim)
        cols = heads_dev * v_dim
        dwo = grad_wo(o_all, grad_out, cols, tp_rank.astype(jnp.int32).reshape(1))
        grad_w_o = (dwo + lax.ppermute(dwo, 'cp', swap_pairs)).reshape(heads_dev, v_dim, dim)

        dw_cat = jnp.einsum('btq,btd->qd', grad_raw, hidden, preferred_element_type=F32)
        grad_w_dq, dw_dkv = join_cp(dw_cat, lax.ppermute(dw_cat, 'cp', swap_pairs), q_lora)
        grad_hidden = jnp.einsum('btq,dq->btd', grad_raw, w_cat, preferred_element_type=F32).astype(BF16)
        return (attn_out, grad_hidden, grad_w_dq, grad_g[:q_lora], dw_dkv.T, grad_g[q_lora:], grad_w_uq, grad_w_uk, grad_w_uv, grad_w_o)

    seq_spec = P(None, 'cp', None)
    full_spec = P()
    head_spec = P(None, 'tp', None)
    out_head_spec = P('tp', None, None)
    all_specs = (seq_spec, seq_spec, full_spec, full_spec, full_spec, full_spec, head_spec, head_spec, head_spec, out_head_spec)
    return jax.shard_map(per_device, mesh=mesh, in_specs=all_specs, out_specs=all_specs, check_vma=False)
```

```python
import functools

import jax
import jax.numpy as jnp
from jax import lax
from jax.experimental import pallas as pl
from jax.experimental.pallas import tpu as pltpu
from jax.sharding import PartitionSpec as P


EPS = 1e-6
THETA = 10000.0
NEG_BIG = -1e30
LOG2E = 1.4426950408889634
F32 = jnp.float32
BF16 = jnp.bfloat16
LANES = 128
GROUP = 4
VMEM_LIMIT = 56 * 1024 * 1024

NN = (((1,), (0,)), ((), ()))
NT = (((1,), (1,)), ((), ()))


def mm(a, b, dims=NN):
    return lax.dot_general(a, b, dims, preferred_element_type=F32)


def rope_tables(positions, rope_dim):
    inv_freq = 1.0 / (THETA ** (jnp.arange(rope_dim // 2, dtype=F32) * 2.0 / rope_dim))
    angles = positions.astype(F32)[:, None] * inv_freq[None, :]
    return jnp.cos(angles), jnp.sin(angles)


def apply_rope(values, cos_tab, sin_tab):
    half_dim = values.shape[-1] // 2
    lead_half = values[..., :half_dim]
    tail_half = values[..., half_dim:]
    return jnp.concatenate([lead_half * cos_tab - tail_half * sin_tab, tail_half * cos_tab + lead_half * sin_tab], axis=-1)


def unrope(grad_vals, cos_tab, sin_tab):
    half_dim = grad_vals.shape[-1] // 2
    lead_half = grad_vals[..., :half_dim]
    tail_half = grad_vals[..., half_dim:]
    return jnp.concatenate([lead_half * cos_tab + tail_half * sin_tab, tail_half * cos_tab - lead_half * sin_tab], axis=-1)


def norm_f32(raw_vals, gain_vec):
    inv_rms = lax.rsqrt(jnp.mean(raw_vals * raw_vals, axis=-1, keepdims=True) + EPS)
    return raw_vals * inv_rms * gain_vec


def attn_kernel(grad, first, scale, *refs):
    it = iter(refs)

    def take(n):
        return [next(it) for _ in range(n)]

    rank_ref, qn_ref, qp_ref, ckv_ref, ckvt_ref, kpe_ref, wuk_ref, wuv_ref, cos_ref, sin_ref = take(10)
    if grad:
        do_ref, kpet_ref = take(2)
        if not first:
            dwk_in, dwv_in = take(6)[:2]
    o_ref = next(it)
    if grad:
        dqn_ref, dqp_ref, dc_ref, dkp_ref, dwk_ref, dwv_ref = take(6)
    k_s, vt_s, e_s, p_s, qm_s = take(5)
    if grad:
        kt_s, v_s, g_s, ds_s, dom_s, dk_s, dv_s, dqp_s = take(8)

    qrows = qn_ref.shape[1]
    blk = qrows // 2
    sub = blk // 2
    half = LANES // 2
    quarter = LANES // 4
    lane = lax.broadcasted_iota(jnp.int32, (1, LANES), 1)
    lane2 = lax.broadcasted_iota(jnp.int32, (1, 2 * LANES), 1)
    coef = scale * LOG2E

    ckv = ckv_ref[0]
    ckvt = ckvt_ref[0]
    wuk = wuk_ref[...]
    wuv = wuv_ref[...]
    k_s[...] = mm(ckv, wuk, NT).astype(BF16)
    vt_s[...] = mm(wuv, ckvt).astype(BF16)
    if grad:
        kt_s[...] = mm(wuk, ckvt).astype(BF16)
        v_s[...] = mm(ckv, wuv, NT).astype(BF16)

    def swap(u):
        shift = quarter // 2
        return jnp.where(lane % quarter < shift, pltpu.roll(u, LANES - shift, 1), pltpu.roll(u, shift, 1))

    qpu = qp_ref[0].astype(F32)
    cos = cos_ref[...]
    sin = sin_ref[...]
    qpr = (qpu * cos + swap(qpu) * sin).astype(BF16)
    zero = jnp.zeros((), BF16)

    def pair_lanes(h):
        return slice(h // 2 * LANES, h // 2 * LANES + LANES)

    for h in range(GROUP):
        qm_s[h, :, :LANES] = jnp.where(lane // half == h % 2, qn_ref[0, :, pair_lanes(h)], zero)
        qm_s[h, :, LANES:] = jnp.where(lane // quarter == h, qpr, zero)
        if grad:
            dom_s[h] = jnp.where(lane2 // half == h, do_ref[0], zero)

    def fold(x, op):
        return op(x.reshape(x.shape[0] // 8, 8, x.shape[1]), axis=0)

    def run(lo, hi):
        units = [(qrows - blk, hi * blk, h) for h in range(GROUP)] + [(0, lo * blk, h) for h in range(GROUP)]

        def scores(i):
            row0, nk, h = units[i]
            kop = jnp.concatenate([k_s[:nk, pair_lanes(h)], kpe_ref[0, :nk, :]], axis=1)
            e_s[i % 2, :nk, :] = mm(kop, qm_s[h, row0:row0 + blk, :], NT)

        def dprobs(i):
            row0, nk, h = units[i]
            g_s[i % 2, :nk, :] = mm(v_s[:nk, pair_lanes(h)], dom_s[h, row0:row0 + blk, pair_lanes(h)], NT)

        def vector_passes(i):
            _, nk, h = units[i]
            slot = i % 2
            st = {}
            cols = slice(h * blk, h * blk + blk)

            def put(key, val, op):
                st[key] = op(st[key], val) if key in st else val

            def top(c):
                x = e_s[slot, c:c + sub, :]
                if c >= nk - blk:
                    key = lax.broadcasted_iota(jnp.int32, (sub, blk), 0) + (c - nk + blk)
                    x = jnp.where(key <= lax.broadcasted_iota(jnp.int32, (sub, blk), 1), x, NEG_BIG)
                    e_s[slot, c:c + sub, :] = x
                put('m', fold(x, jnp.max), jnp.maximum)

            def expo(c):
                if c == 0:
                    st['max'] = jnp.max(st['m'], axis=0, keepdims=True)
                e = jnp.exp2((e_s[slot, c:c + sub, :] - st['max']) * coef)
                e_s[slot, c:c + sub, :] = e
                put('l', fold(e, jnp.sum), jnp.add)
                if grad:
                    put('d', fold(e * g_s[slot, c:c + sub, :], jnp.sum), jnp.add)

            def probs(c):
                if c == 0:
                    st['inv'] = 1.0 / jnp.sum(st['l'], axis=0, keepdims=True)
                    if grad:
                        st['dot'] = jnp.sum(st['d'], axis=0, keepdims=True) * st['inv']
                p = e_s[slot, c:c + sub, :] * st['inv']
                p_s[c:c + sub, cols] = p.astype(BF16)
                if grad:
                    ds_s[c:c + sub, cols] = (p * (g_s[slot, c:c + sub, :] - st['dot'])).astype(BF16)

            return [functools.partial(f, c) for f in (top, expo, probs) for c in range(0, nk, sub)]

        def out(i):
            row0, nk, h = units[i]
            parts = [mm(vt_s[g * half:g * half + half, :nk], p_s[:nk, g * blk:g * blk + blk]) for g in (h - 1, h)]
            o_ref[0, row0:row0 + blk, pair_lanes(h)] = jnp.concatenate(parts, axis=0).T.astype(BF16)

        def dquery(i):
            row0, nk, h = units[i]
            rows = slice(row0, row0 + blk)
            parts = []
            for g in (h - 1, h):
                kop_t = jnp.concatenate([kt_s[g * half:g * half + half, :nk], kpet_ref[0, :, :nk]], axis=0)
                dq = mm(kop_t, ds_s[:nk, g * blk:g * blk + blk])
                parts.append(dq[:half])
                dqp_s[g * quarter:g * quarter + quarter, :] = dq[half:]
            dqn_ref[0, rows, pair_lanes(h)] = (jnp.concatenate(parts, axis=0).T * scale).astype(BF16)
            if h == GROUP - 1:
                dqp = dqp_s[...].T * scale
                dqp_ref[0, rows, :] = (dqp * cos_ref[rows, :] - swap(dqp) * sin_ref[rows, :]).astype(BF16)

        def dkeys(i, dst, lhs, rhs):
            row0, nk, h = units[i]
            cols = slice((h - 1) * blk, (h + 1) * blk)
            val = mm(lhs[:nk, cols], jnp.concatenate([rhs[h - 1, row0:row0 + blk, :], rhs[h, row0:row0 + blk, :]], axis=0))
            if row0:
                dst[h // 2, :nk, :] = val
                if nk < dst.shape[1]:
                    dst[h // 2, nk:, :] = jnp.zeros((dst.shape[1] - nk, dst.shape[2]), F32)
            else:
                dst[h // 2, :nk, :] += val

        def before(i):
            return [functools.partial(scores, i)] + ([functools.partial(dprobs, i)] if grad else [])

        def after(i):
            return [functools.partial(out, i)] + ([functools.partial(dquery, i)] if grad else [])

        def after_keys(i):
            return [functools.partial(dkeys, i, dv_s, p_s, dom_s), functools.partial(dkeys, i, dk_s, ds_s, qm_s)] if grad else []

        def region(i):
            for u in (i, i + 1):
                vec = vector_passes(u)
                mat = before(u + 1) if u + 1 < len(units) else []
                if i:
                    mat = mat + (after(i - 1) if u == i else after_keys(i - 1))
                for c, f in enumerate(vec):
                    for g in mat[c * len(mat) // len(vec):(c + 1) * len(mat) // len(vec)]:
                        g()
                    f()

        for f in before(0):
            f()
        for i in range(0, len(units), 2):
            region(i)
        for f in after(len(units) - 1) + after_keys(len(units) - 1):
            f()

    rank = rank_ref[0]

    @pl.when(rank == 0)
    def _():
        run(1, 4)

    @pl.when(rank == 1)
    def _():
        run(2, 3)

    if grad:
        dkb = (jnp.concatenate([dk_s[0, :, :LANES], dk_s[1, :, :LANES]], axis=1) * scale).astype(BF16)
        dvb = (dv_s[0] + dv_s[1]).astype(BF16)
        dkp = (dk_s[0, :, LANES:] + dk_s[1, :, LANES:]) * scale
        dc = mm(dkb, wuk) + mm(dvb, wuv)
        dwk = mm(ckvt, dkb)
        dwv = mm(ckvt, dvb)
        dwk_ref[...] = dwk if first else dwk_in[...] + dwk
        dwv_ref[...] = dwv if first else dwv_in[...] + dwv
        step = pl.program_id(0)

        @pl.when(step == 0)
        def _():
            dc_ref[0] = dc
            dkp_ref[0] = dkp

        @pl.when(step > 0)
        def _():
            dc_ref[0] += dc
            dkp_ref[0] += dkp


def attention(j, grad_args, prev, scale, rank_arr, qn, qp, ckv, ckvt, kpe4, wuk, wuv, cos, sin):
    nb, qrows, width = qn.shape
    nkeys, latent = ckv.shape[1:]
    step = GROUP * LANES // 2
    groups = width // step
    blk = qrows // 2
    grad = grad_args is not None
    first = prev is None

    def row(cols, at=j):
        return pl.BlockSpec((1, qrows, cols), lambda i: (at, 0, i))

    def whole(*shape):
        return pl.BlockSpec((1, *shape), lambda i: (j, 0, 0))

    weight = pl.BlockSpec((step, latent), lambda i: (i, 0))
    table = pl.BlockSpec((qrows, LANES), lambda i: (0, 0))
    dweight = pl.BlockSpec((latent, step), lambda i: (0, i))
    in_specs = [pl.BlockSpec(memory_space=pltpu.SMEM), row(step), row(LANES), whole(nkeys, latent), whole(latent, nkeys), whole(nkeys, LANES), weight, weight, table, table]
    args = [rank_arr, qn, qp, ckv, ckvt, kpe4, wuk, wuv, cos, sin]
    out_specs = [row(step, 0)]
    out_shape = [jax.ShapeDtypeStruct((1, qrows, width), BF16)]
    scratch = [
        pltpu.VMEM((nkeys, step), BF16), pltpu.VMEM((step, nkeys), BF16), pltpu.VMEM((2, nkeys, blk), F32),
        pltpu.VMEM((nkeys, GROUP * blk), BF16), pltpu.VMEM((GROUP, qrows, step), BF16),
    ]
    aliases = {}
    if grad:
        in_specs += [row(step), whole(LANES // 4, nkeys)]
        args += grad_args
        if not first:
            dqn, dqp, dc, dkp, dwk, dwv = prev
            base = len(args)
            in_specs += [dweight] * 2 + [pl.BlockSpec(memory_space=pl.ANY)] * 4
            args += [dwk, dwv, dqn, dqp, dc, dkp]
            aliases = {base + i: o for i, o in enumerate((5, 6, 1, 2, 3, 4))}
        out_specs += [row(step), row(LANES), whole(nkeys, latent), whole(nkeys, LANES), dweight, dweight]
        out_shape += [
            jax.ShapeDtypeStruct((nb, qrows, width), BF16), jax.ShapeDtypeStruct((nb, qrows, width // 2), BF16),
            jax.ShapeDtypeStruct((nb, nkeys, latent), F32), jax.ShapeDtypeStruct((nb, nkeys, LANES), F32),
            jax.ShapeDtypeStruct((latent, width), F32), jax.ShapeDtypeStruct((latent, width), F32),
        ]
        scratch += [
            pltpu.VMEM((step, nkeys), BF16), pltpu.VMEM((nkeys, step), BF16), pltpu.VMEM((2, nkeys, blk), F32),
            pltpu.VMEM((nkeys, GROUP * blk), BF16), pltpu.VMEM((GROUP, qrows, step), BF16),
            pltpu.VMEM((2, nkeys, step), F32), pltpu.VMEM((2, nkeys, step), F32), pltpu.VMEM((LANES, blk), F32),
        ]
    pairs = 5 * GROUP * groups * blk * blk
    return pl.pallas_call(
        functools.partial(attn_kernel, grad, first, scale),
        grid=(groups,),
        in_specs=in_specs,
        out_specs=out_specs,
        out_shape=out_shape,
        scratch_shapes=scratch,
        input_output_aliases=aliases,
        name="attn_fwd_bwd" if grad else "attn_fwd",
        compiler_params=pltpu.CompilerParams(dimension_semantics=("arbitrary",), vmem_limit_bytes=VMEM_LIMIT),
        cost_estimate=pl.CostEstimate(flops=pairs * step * (12 if grad else 4), bytes_accessed=20 * nb * qrows * width, transcendentals=pairs),
    )(*args)


def place_kernel(src_ref, y_ref):
    for t in range(src_ref.shape[0]):
        y_ref[t, 0] = src_ref[t]


def place(nb, src):
    tp, rows, dim = src.shape
    tile = 4 * LANES
    return pl.pallas_call(
        place_kernel,
        grid=(dim // tile,),
        in_specs=[pl.BlockSpec((tp, rows, tile), lambda i: (0, 0, i))],
        out_specs=pl.BlockSpec((tp, 1, rows, tile), lambda i: (0, 0, 0, i)),
        out_shape=jax.ShapeDtypeStruct((tp, nb, rows, dim), src.dtype),
        name="place",
        compiler_params=pltpu.CompilerParams(dimension_semantics=("arbitrary",), vmem_limit_bytes=VMEM_LIMIT),
        cost_estimate=pl.CostEstimate(flops=4 * tp * rows * dim, bytes_accessed=4 * tp * rows * dim, transcendentals=0),
    )(src)


def out_kernel(o_ref, w_ref, *rest):
    y_ref = rest[-1]
    w = w_ref[...]
    for t in range(o_ref.shape[0]):
        y_ref[t, 0] = mm(o_ref[t], w).astype(BF16)


def out_proj(j, nb, o_all, w_o, prev):
    tp, rows, width = o_all.shape
    dim = w_o.shape[1]
    tile = 4 * LANES
    in_specs = [pl.BlockSpec((tp, rows, width), lambda i: (0, 0, 0)), pl.BlockSpec((width, tile), lambda i: (0, i))]
    args = [o_all, w_o]
    aliases = {}
    if prev is not None:
        in_specs.append(pl.BlockSpec(memory_space=pl.ANY))
        args.append(prev)
        aliases = {2: 0}
    return pl.pallas_call(
        out_kernel,
        grid=(dim // tile,),
        in_specs=in_specs,
        out_specs=pl.BlockSpec((tp, 1, rows, tile), lambda i: (0, j, 0, i)),
        out_shape=jax.ShapeDtypeStruct((tp, nb, rows, dim), BF16),
        input_output_aliases=aliases,
        name="out_proj",
        compiler_params=pltpu.CompilerParams(dimension_semantics=("arbitrary",), vmem_limit_bytes=VMEM_LIMIT),
        cost_estimate=pl.CostEstimate(flops=2 * tp * rows * width * dim, bytes_accessed=2 * (2 * tp * rows * width + width * dim), transcendentals=0),
    )(*args)


def dwo_kernel(tp, col_ref, *refs):
    *o_refs, dy_ref, out_ref, ot_s = refs
    step = pl.program_id(0)
    per = o_refs[0].shape[0]
    rows = o_refs[0].shape[1]
    for j, o_ref in enumerate(o_refs):
        @pl.when(step // (tp // per) == j)
        def _():
            for t in range(per):
                ot_s[:, t * rows:(t + 1) * rows] = o_ref[t].astype(F32).T.astype(BF16)

    tile = 4 * LANES
    for n in range(0, out_ref.shape[1], tile):
        cols = slice(n, n + tile)
        val = mm(ot_s[...], jnp.concatenate([dy_ref[t, 0, :, cols] for t in range(per)], axis=0))

        @pl.when(step == 0)
        def _():
            out_ref[:, cols] = val

        @pl.when(step > 0)
        def _():
            out_ref[:, cols] += val


def grad_wo(o_all, dy, cols, col_arr):
    tp, rows, _ = o_all[0].shape
    nb = len(o_all)
    dim = dy.shape[-1]
    per = tp
    turns = tp // per

    def o_spec(j):
        whole = o_all[j].shape[2] == cols
        return pl.BlockSpec((per, rows, cols), lambda i, col: (jnp.clip(i - j * turns, 0, turns - 1), 0, 0 if whole else col[0]))

    return pl.pallas_call(
        functools.partial(dwo_kernel, tp),
        grid_spec=pltpu.PrefetchScalarGridSpec(
            num_scalar_prefetch=1,
            grid=(nb * turns,),
            in_specs=[o_spec(j) for j in range(nb)] + [pl.BlockSpec((per, 1, rows, dim), lambda i, col: (i % turns, i // turns, 0, 0))],
            out_specs=pl.BlockSpec((cols, dim), lambda i, col: (0, 0)),
            scratch_shapes=[pltpu.VMEM((cols, per * rows), BF16)],
        ),
        out_shape=jax.ShapeDtypeStruct((cols, dim), F32),
        name="grad_wo",
        compiler_params=pltpu.CompilerParams(dimension_semantics=("arbitrary",), vmem_limit_bytes=VMEM_LIMIT * 9 // 8),
        cost_estimate=pl.CostEstimate(flops=2 * nb * tp * rows * cols * dim, bytes_accessed=2 * nb * tp * rows * (cols + dim), transcendentals=0),
    )(col_arr, *o_all, dy.reshape(tp, nb, rows, dim))


def join_kernel(a_ref, b_ref, q_ref, kv_ref):
    split = q_ref.shape[1]
    q_ref[...] = (a_ref[:split, :] + b_ref[:split, :]).T
    kv_ref[...] = a_ref[split:, :] + b_ref[split:, :]


def join_cp(a, b, split):
    wide, dim = a.shape
    tile = 2 * LANES
    part = pl.BlockSpec((wide, tile), lambda i: (0, i))
    return pl.pallas_call(
        join_kernel,
        grid=(dim // tile,),
        in_specs=[part, part],
        out_specs=[pl.BlockSpec((tile, split), lambda i: (i, 0)), pl.BlockSpec((wide - split, tile), lambda i: (0, i))],
        out_shape=[jax.ShapeDtypeStruct((dim, split), F32), jax.ShapeDtypeStruct((wide - split, dim), F32)],
        name="join_cp",
        compiler_params=pltpu.CompilerParams(dimension_semantics=("arbitrary",), vmem_limit_bytes=VMEM_LIMIT),
        cost_estimate=pl.CostEstimate(flops=wide * dim, bytes_accessed=12 * wide * dim, transcendentals=0),
    )(a, b)


def solution(mesh):
    cp_size = mesh.shape['cp']
    tp_size = mesh.shape['tp']
    swap_pairs = [(0, 1), (1, 0)]

    def per_device(hidden, grad_out, w_dq, g_q, w_dkv, g_kv, w_uq, w_uk, w_uv, w_o):
        cp_rank = lax.axis_index('cp')
        tp_rank = lax.axis_index('tp')
        n_batch, seq_local, dim = hidden.shape
        nb = n_batch // tp_size
        q_lora = w_dq.shape[1]
        kv_lora = g_kv.shape[0]
        nope = w_uk.shape[2]
        qk_dim = w_uq.shape[2]
        rope_dim = qk_dim - nope
        heads_dev = w_uq.shape[1]
        heads = heads_dev * tp_size
        v_dim = w_uv.shape[2]
        scale = qk_dim ** -0.5
        half_len = seq_local // 2
        half_heads = heads_dev // 2

        def swapped(val):
            return lax.ppermute(val, 'cp', swap_pairs)

        def shifted(val, k):
            return lax.ppermute(val, 'tp', [(s, (s + k) % tp_size) for s in range(tp_size)])

        def own_half(w):
            return lax.dynamic_slice_in_dim(w, cp_rank * half_heads, half_heads, 0)

        def gather_weight(half):
            return lax.all_gather(half, ('tp', 'cp'), axis=0, tiled=True)

        slabs = q_lora // kv_lora
        wq_rows = own_half(jnp.transpose(w_uq, (1, 2, 0)))
        up_rows = [wq_rows[..., s * kv_lora:(s + 1) * kv_lora] for s in range(slabs)]
        up_rows += [own_half(jnp.transpose(w, (1, 2, 0))) for w in (w_uk, w_uv)]
        w_up = gather_weight(jnp.concatenate(up_rows, axis=1))
        wo_all = gather_weight(own_half(w_o)).reshape(heads * v_dim, dim)

        def q_rows(lo, hi):
            parts = [w_up[:, s * qk_dim + lo:s * qk_dim + hi] for s in range(slabs)]
            return jnp.concatenate(parts, axis=2).reshape(heads * (hi - lo), q_lora)

        wqn = q_rows(0, nope)
        wqp = q_rows(nope, qk_dim)
        wuk = w_up[:, slabs * qk_dim:slabs * qk_dim + nope].reshape(heads * nope, kv_lora)
        wuv = w_up[:, slabs * qk_dim + nope:].reshape(heads * v_dim, kv_lora)

        local_idx = jnp.arange(seq_local, dtype=jnp.int32)
        block_id = jnp.where(local_idx < half_len, cp_rank, 2 * cp_size - 1 - cp_rank)
        positions = block_id * half_len + local_idx % half_len
        cos_tab, sin_tab = rope_tables(positions, rope_dim)
        cos128 = jnp.tile(cos_tab, (1, 8))
        sin128 = jnp.tile(jnp.concatenate([-sin_tab, sin_tab], axis=1), (1, 4))

        w_cat = jnp.concatenate([w_dq, w_dkv], axis=1)
        x_own = lax.dynamic_slice_in_dim(hidden, tp_rank * nb, nb, 0)
        dy_own = lax.dynamic_slice_in_dim(grad_out, tp_rank * nb, nb, 0)

        raw = jnp.einsum('btd,dq->btq', x_own, w_cat, preferred_element_type=F32).astype(BF16)
        cq_f32 = raw[..., :q_lora].astype(F32)
        ckv_f32 = raw[..., q_lora:q_lora + kv_lora].astype(F32)
        gq_f32 = g_q.astype(F32)
        gkv_f32 = g_kv.astype(F32)
        c_q = norm_f32(cq_f32, gq_f32).astype(BF16)
        c_kv = norm_f32(ckv_f32, gkv_f32).astype(BF16)
        k_pe = apply_rope(raw[..., q_lora + kv_lora:].astype(F32), cos_tab, sin_tab).astype(BF16)

        def by_position(own, other):
            lo = jnp.where(cp_rank == 0, own[:, :half_len], other[:, :half_len])
            lo2 = jnp.where(cp_rank == 0, other[:, :half_len], own[:, :half_len])
            hi = jnp.where(cp_rank == 0, other[:, half_len:], own[:, half_len:])
            hi2 = jnp.where(cp_rank == 0, own[:, half_len:], other[:, half_len:])
            return jnp.concatenate([lo, lo2, hi, hi2], axis=1)

        other_kv, other_pe = lax.ppermute((c_kv, k_pe), 'cp', swap_pairs)
        ckv_seq = by_position(c_kv, other_kv)
        kpe_seq = by_position(k_pe, other_pe)
        ckvt_seq = jnp.swapaxes(ckv_seq, 1, 2)
        kpet_seq = jnp.swapaxes(kpe_seq, 1, 2)
        kpe4 = jnp.tile(kpe_seq, (1, 1, 4))

        qn = jnp.einsum('btq,fq->btf', c_q, wqn, preferred_element_type=F32).astype(BF16)
        qp = jnp.einsum('btq,fq->btf', c_q, wqp, preferred_element_type=F32).astype(BF16)
        grad_o = jnp.einsum('btd,fd->btf', dy_own, wo_all, preferred_element_type=F32).astype(BF16)

        rank_arr = cp_rank.astype(jnp.int32).reshape(1)
        attn_args = (rank_arr, qn, qp, ckv_seq, ckvt_seq, kpe4, wuk, wuv, cos128, sin128)
        prev = None
        cols = heads_dev * v_dim
        o_all = [None] * nb
        o_first = attention(0, None, None, scale, *attn_args)[0]
        own_cols = [lax.dynamic_slice_in_dim(o_first[0], (tp_rank + k) % tp_size * cols, cols, 1) for k in range(tp_size)]
        own_cols = own_cols[:1] + [shifted(own_cols[k], k) for k in range(1, tp_size)]
        y_first = jnp.einsum('btf,fd->btd', o_first, wo_all, preferred_element_type=F32).astype(BF16)
        y_first = lax.all_gather(y_first, 'tp', axis=0, tiled=True)
        for j in (*range(1, nb), 0):
            res = attention(j, [grad_o, kpet_seq], prev, scale, *attn_args)
            prev = res[1:]
            if j:
                o_all[j] = lax.all_gather(res[0], 'tp', axis=0, tiled=True)
        dqn, dqp, dc_seq, dkp_seq, dwk, dwv = prev

        dkp_seq = dkp_seq[..., :32] + dkp_seq[..., 32:64] + dkp_seq[..., 64:96] + dkp_seq[..., 96:]
        lat = jnp.concatenate([dc_seq, dkp_seq], axis=-1)
        b0, b1, b2, b3 = (lat[:, i * half_len:(i + 1) * half_len] for i in range(4))
        outer = jnp.concatenate([b0, b3], axis=1)
        inner = jnp.concatenate([b1, b2], axis=1)
        mine = jnp.where(cp_rank == 0, outer, inner)
        theirs = jnp.where(cp_rank == 0, inner, outer)
        lat = mine + lax.ppermute(theirs, 'cp', swap_pairs)
        grad_cq = jnp.einsum('btf,fq->btq', dqn, wqn, preferred_element_type=F32) + jnp.einsum('btf,fq->btq', dqp, wqp, preferred_element_type=F32)

        norm_q_pull = jax.vjp(norm_f32, cq_f32, gq_f32)[1]
        grad_cq_raw, grad_g_q = norm_q_pull(grad_cq)
        norm_kv_pull = jax.vjp(norm_f32, ckv_f32, gkv_f32)[1]
        grad_ckv_raw, grad_g_kv = norm_kv_pull(lat[..., :kv_lora])
        grad_raw = jnp.concatenate([grad_cq_raw, grad_ckv_raw, unrope(lat[..., kv_lora:], cos_tab, sin_tab)], axis=-1).astype(BF16)
        grad_raw = lax.all_gather(grad_raw, 'tp', axis=0, tiled=True)
        part = jnp.concatenate([grad_g_q, grad_g_kv])
        part = part + swapped(part)
        parts = jnp.stack([part] + [shifted(part, k) for k in range(1, tp_size)])
        grad_g = sum(lax.dynamic_index_in_dim(parts, (tp_rank - s) % tp_size, 0, keepdims=False) for s in range(tp_size))

        q_half = q_lora // 2
        cq_mine = lax.dynamic_slice_in_dim(c_q, cp_rank * q_half, q_half, 2)
        cq_theirs = lax.dynamic_slice_in_dim(c_q, (1 - cp_rank) * q_half, q_half, 2)

        def dw_of(dq, cq):
            return jnp.einsum('btf,btq->fq', dq, cq, preferred_element_type=F32)

        dwqn = dw_of(dqn, cq_mine) + swapped(dw_of(dqn, cq_theirs))
        dwqp = dw_of(dqp, cq_mine) + swapped(dw_of(dqp, cq_theirs))
        c_half = kv_lora // 2
        dw_kv = jnp.stack([dwk, dwv])
        kv_mine = lax.dynamic_slice_in_dim(dw_kv, cp_rank * c_half, c_half, 1)
        kv_theirs = lax.dynamic_slice_in_dim(dw_kv, (1 - cp_rank) * c_half, c_half, 1)
        dw_kv = kv_mine + swapped(kv_theirs)
        dwqn = lax.psum_scatter(dwqn, 'tp', scatter_dimension=0, tiled=True)
        dwqp = lax.psum_scatter(dwqp, 'tp', scatter_dimension=0, tiled=True)
        dw_kv = lax.psum_scatter(dw_kv, 'tp', scatter_dimension=2, tiled=True)
        dwq = jnp.concatenate([dwqn.reshape(heads_dev, nope, q_half), dwqp.reshape(heads_dev, rope_dim, q_half)], axis=1)

        def join(part, axis):
            other = swapped(part)
            return jnp.concatenate([jnp.where(cp_rank == 0, part, other), jnp.where(cp_rank == 0, other, part)], axis=axis)

        grad_w_uq = jnp.transpose(join(dwq, 2), (2, 0, 1))
        dw_kv = join(dw_kv, 1)
        grad_w_uk = dw_kv[0].reshape(kv_lora, heads_dev, nope)
        grad_w_uv = dw_kv[1].reshape(kv_lora, heads_dev, v_dim)

        y = place(nb, y_first)
        for j in range(1, nb):
            y = out_proj(j, nb, o_all[j], wo_all, y)
        own_cols = jnp.stack(own_cols)
        o_all[0] = jnp.stack([lax.dynamic_index_in_dim(own_cols, (tp_rank - s) % tp_size, 0, keepdims=False) for s in range(tp_size)])
        attn_out = y.reshape(n_batch, seq_local, dim)
        dwo = grad_wo(o_all, grad_out, cols, tp_rank.astype(jnp.int32).reshape(1))
        grad_w_o = (dwo + lax.ppermute(dwo, 'cp', swap_pairs)).reshape(heads_dev, v_dim, dim)

        dw_cat = jnp.einsum('btq,btd->qd', grad_raw, hidden, preferred_element_type=F32)
        dw_other = lax.ppermute(dw_cat, 'cp', swap_pairs)
        grad_w_dq, dw_dkv = join_cp(dw_cat, dw_other, q_lora)
        grad_hidden = jnp.einsum('btq,dq->btd', grad_raw, w_cat, preferred_element_type=F32).astype(BF16)
        return (attn_out, grad_hidden, grad_w_dq, grad_g[:q_lora], dw_dkv.T, grad_g[q_lora:], grad_w_uq, grad_w_uk, grad_w_uv, grad_w_o)

    seq_spec = P(None, 'cp', None)
    full_spec = P()
    head_spec = P(None, 'tp', None)
    out_head_spec = P('tp', None, None)
    all_specs = (seq_spec, seq_spec, full_spec, full_spec, full_spec, full_spec, head_spec, head_spec, head_spec, out_head_spec)
    return jax.shard_map(per_device, mesh=mesh, in_specs=all_specs, out_specs=all_specs, check_vma=False)
```
